512 devices in a mesh: seq: 128 (over z, y, core), head: 4 (over x).
Axes of the slice: x: 4, y: 8, z: 8, core: 2. Of those that a mesh axis runs over, the one named last changes fastest.
Arguments:
- hidden_states: bfloat16 [32768, 2048], P('seq', 'head'), may hold values from -0.375 to 0.375
- w_lambda: bfloat16 [2048, 512], P('head'), may hold values from -2 to 2
- queries: bfloat16 [32768, 2048], P('seq', 'head'), may hold values from -6 to 6
- keys: bfloat16 [32768, 2048], P('seq', 'head'), may hold values from -0.01171875 to 0.01171875
- values: bfloat16 [32768, 4096], P('seq', 'head'), may hold values from -6 to 6
- d_out: bfloat16 [32768, 4096], P('seq', 'head'), may hold values from -0.75 to 0.75
- d_state: float32 [32, 64, 128], P('head'), may hold values from -6 to 6
Outputs:
- out: bfloat16 [32768, 4096], P('seq', 'head')
- d_queries: bfloat16 [32768, 2048], P('seq', 'head')
- d_keys: bfloat16 [32768, 2048], P('seq', 'head')
- d_values: bfloat16 [32768, 4096], P('seq', 'head')
- d_hidden: bfloat16 [32768, 2048], P('seq', 'head')
- d_w_lambda: float32 [2048, 512], P(('head', 'seq'))
The draws below stay inside these ranges and needn't reach their ends.
All inputs are finite; a program needn't handle non-finite values.
Results may differ from the reference program's by a relative error of at most 0.0049.
Values may be sent and summed in bfloat16 or wider, within the bound.
A program may use at most 64 MiB of HBM per device.

```python
import jax
import jax.numpy as jnp
from jax import lax

D = 2048
H = 32
DK = 64
DV = 128
TOK_DEV = 256
TOKENS = 32768
TOK_BITS = 8
SEQ_BITS = 7
LEVELS = 16
N_SEQ = 128
N_HEAD = 4


def block_scale(key, dims, cuts, smallest, top_value):
    def one(axis_at, parts):
        heights = jax.random.uniform(jax.random.fold_in(jax.random.fold_in(key, 6), axis_at), (parts,), jnp.float32, smallest / len(cuts), top_value / len(cuts))
        return jnp.repeat(jnp.exp(heights), dims[axis_at] // parts).reshape((-1,) + (1,) * (len(dims) - axis_at - 1))

    loudness = one(*cuts[0])
    for cut in cuts[1:]:
        loudness = loudness * one(*cut)
    return loudness


def noise(rng, extent, scale, bound, pieces=(), held_as=jnp.bfloat16):
    array = scale * jax.random.normal(rng, extent, jnp.float32)
    if pieces:
        array = array * block_scale(rng, extent, pieces, -0.22, 0.18)
    return jnp.clip(array, -bound, bound).astype(held_as)


def setup_inputs(seed: int = 0) -> dict:
    streams_of = jax.random.split(jax.random.key(seed), 8)
    return {
        "hidden_states": noise(streams_of[0], (TOKENS, D), 0.0625, 0.375, ((0, 128), (1, 4))),
        "w_lambda": noise(streams_of[1], (D, H * LEVELS), (D // 256) ** -0.5, 2.0, ((0, 4),)),
        "queries": noise(streams_of[2], (TOKENS, H * DK), 1.0, 6.0, ((0, 128), (1, 4))),
        "keys": noise(streams_of[3], (TOKENS, H * DK), (DK * TOKENS // 8) ** -0.5, 0.01171875, ((0, 128), (1, 4))),
        "values": noise(streams_of[4], (TOKENS, H * DV), 1.0, 6.0, ((0, 128), (1, 4))),
        "d_out": noise(streams_of[5], (TOKENS, H * DV), 0.125, 0.75, ((0, 128), (1, 4))),
        "d_state": noise(streams_of[6], (H, DK, DV), 1.0, 6.0, ((0, 4),), jnp.float32),
    }


PRECISE = lax.Precision.HIGHEST


def digit_count(values, width):
    total = jnp.zeros_like(values)
    for shift in range(width):
        total = total + ((values >> shift) > 0).astype(jnp.int32)
    return total


def level_table(row_count, width, levels):
    later = jnp.arange(row_count, dtype=jnp.int32)[:, None]
    earlier = jnp.arange(row_count, dtype=jnp.int32)[None, :]
    depth = digit_count(jnp.bitwise_xor(later, earlier), width)
    keep = earlier <= later
    grid = jnp.arange(levels, dtype=jnp.int32)[:, None, None]
    return jnp.where((depth[None] == grid) & keep[None], 1.0, 0.0).astype(jnp.float32)


def pick_table(width, seq_bits, levels):
    wanted = width + 1 + jnp.arange(seq_bits, dtype=jnp.int32)
    return jnp.where(jnp.arange(levels, dtype=jnp.int32)[None, :] == wanted[:, None], 1.0, 0.0).astype(jnp.float32)


def swap_blocks(stack, bit):
    count = stack.shape[0]
    folded = stack.reshape((count >> (bit + 1), 2, 1 << bit) + stack.shape[1:])
    return folded[:, ::-1].reshape(stack.shape)


def local_pass(query_heads, key_heads, value_heads, level_weights, table, states, picks, grad_heads):
    query_wide = query_heads.astype(jnp.float32)
    key_wide = key_heads.astype(jnp.float32)
    value_wide = value_heads.astype(jnp.float32)
    grad_wide = grad_heads.astype(jnp.float32)
    scores = jnp.einsum('thd,shd->hts', query_wide, key_wide, precision=PRECISE)
    spread = jnp.einsum('thl,lts->hts', level_weights, table, precision=PRECISE)
    mixed = lax.optimization_barrier((scores * spread).astype(jnp.bfloat16))
    mixed_wide = mixed.astype(jnp.float32)
    local_out = jnp.einsum('hts,shv->thv', mixed_wide, value_wide, precision=PRECISE)
    chosen = jnp.einsum('thl,kl->thk', level_weights, picks, precision=PRECISE)
    scaled = chosen[:, :, :, None] * query_wide[:, :, None, :]
    carried = jnp.einsum('thkd,khdv->thv', scaled, states, precision=PRECISE)
    result = (local_out + carried).astype(jnp.bfloat16)
    grad_mixed = jnp.einsum('thv,shv->hts', grad_wide, value_wide, precision=PRECISE)
    grad_values = jnp.einsum('hts,thv->shv', mixed_wide, grad_wide, precision=PRECISE)
    grad_scores = lax.optimization_barrier((grad_mixed * spread).astype(jnp.bfloat16)).astype(jnp.float32)
    grad_weights = jnp.einsum('hts,lts->thl', grad_mixed * scores, table, precision=PRECISE)
    grad_queries = jnp.einsum('hts,shd->thd', grad_scores, key_wide, precision=PRECISE)
    grad_keys = jnp.einsum('hts,thd->shd', grad_scores, query_wide, precision=PRECISE)
    grad_scaled = jnp.einsum('thv,khdv->thkd', grad_wide, states, precision=PRECISE)
    grad_queries = grad_queries + jnp.einsum('thk,thkd->thd', chosen, grad_scaled, precision=PRECISE)
    grad_chosen = jnp.einsum('thkd,thd->thk', grad_scaled, query_wide, precision=PRECISE)
    grad_weights = grad_weights + jnp.einsum('thk,kl->thl', grad_chosen, picks, precision=PRECISE)
    grad_states = jnp.einsum('thkd,thv->khdv', scaled, grad_wide, precision=PRECISE)
    return result, grad_queries, grad_keys, grad_values, grad_weights, grad_states


def reference(hidden_states, w_lambda, queries, keys, values, d_out, d_state):
    projected = jnp.dot(hidden_states, w_lambda, preferred_element_type=jnp.float32)
    weight_all = jax.nn.softplus(projected).reshape(N_SEQ, TOK_DEV, H, LEVELS)
    table = level_table(TOK_DEV, TOK_BITS, LEVELS)
    picks = pick_table(TOK_BITS, SEQ_BITS, LEVELS)
    block_ids = jnp.arange(N_SEQ, dtype=jnp.int32)
    group = H // N_HEAD
    query_all = queries.reshape(N_SEQ, TOK_DEV, H, DK)
    key_all = keys.reshape(N_SEQ, TOK_DEV, H, DK)
    value_all = values.reshape(N_SEQ, TOK_DEV, H, DV)
    grad_all = d_out.reshape(N_SEQ, TOK_DEV, H, DV)
    collected = []
    for start in range(0, H, group):
        query_group = query_all[:, :, start:start + group]
        key_group = key_all[:, :, start:start + group]
        value_group = value_all[:, :, start:start + group]
        weight_group = weight_all[:, :, start:start + group]
        grad_group = grad_all[:, :, start:start + group]
        state_seed = d_state[start:start + group]
        key_wide = key_group.astype(jnp.float32)
        value_wide = value_group.astype(jnp.float32)
        kv_state = jnp.einsum('bthd,bthv->bhdv', key_wide, value_wide, precision=PRECISE)
        total = kv_state
        uppers = []
        for bit in range(SEQ_BITS):
            partner = swap_blocks(total, bit)
            is_upper = ((block_ids >> bit) & 1) == 1
            uppers.append(jnp.where(is_upper[:, None, None, None], partner, 0.0))
            total = total + partner
        states = jnp.stack(uppers, axis=1)

        def one_block(items):
            return local_pass(items[0], items[1], items[2], items[3], table, items[4], picks, items[5])

        result, query_grads, key_grads, value_grads, weight_grads, state_grads = lax.map(
            one_block, (query_group, key_group, value_group, weight_group, states, grad_group))
        adjoint = jnp.zeros_like(kv_state)
        for bit in reversed(range(SEQ_BITS)):
            is_upper = ((block_ids >> bit) & 1) == 1
            pending = adjoint + jnp.where(is_upper[:, None, None, None], state_grads[:, bit], 0.0)
            adjoint = adjoint + swap_blocks(pending, bit)
        adjoint = adjoint + state_seed[None]
        key_grads = key_grads + jnp.einsum('bthv,bhdv->bthd', value_wide, adjoint, precision=PRECISE)
        value_grads = value_grads + jnp.einsum('bthd,bhdv->bthv', key_wide, adjoint, precision=PRECISE)
        collected.append((result, query_grads, key_grads, value_grads, weight_grads))
    joined = [jnp.concatenate([entry[place] for entry in collected], axis=2) for place in range(5)]
    out = joined[0].reshape(TOKENS, H * DV)
    d_queries = joined[1].reshape(TOKENS, H * DK).astype(jnp.bfloat16)
    d_keys = joined[2].reshape(TOKENS, H * DK).astype(jnp.bfloat16)
    d_values = joined[3].reshape(TOKENS, H * DV).astype(jnp.bfloat16)
    grad_level = joined[4].reshape(TOKENS, H * LEVELS)
    grad_projected = (grad_level * jax.nn.sigmoid(projected)).astype(jnp.bfloat16)
    d_hidden = jnp.dot(grad_projected, w_lambda.T, preferred_element_type=jnp.float32).astype(jnp.bfloat16)
    d_w_lambda = jnp.dot(hidden_states.T, grad_projected, preferred_element_type=jnp.float32)
    return (out, d_queries, d_keys, d_values, d_hidden, d_w_lambda)
```

```python
import functools

import jax
import jax.numpy as jnp
import numpy as np
from jax import lax
from jax.experimental import pallas as pl
from jax.experimental.pallas import tpu as pltpu
from jax.sharding import PartitionSpec as P

DK = 64
DV = 128
LEVELS = 16
BASE = 9
T = 256
F32 = jnp.float32
BF16 = jnp.bfloat16


def dot(a, b, da, db):
    return lax.dot_general(a, b, (((da,), (db,)), ((), ())), preferred_element_type=F32)


def mm(a, b):
    return dot(a, b, 1, 0)


def segment_tables():
    select = np.zeros((128, 256), np.float32)
    member = np.zeros((256, 128), np.float32)
    level = np.full((256,), 99, np.int32)
    level[:128] = 0
    rows = np.arange(128)
    select[rows, rows] = 1.0
    member[rows, rows] = 1.0
    col = 128
    for k in range(7):
        for i in range(64 >> k):
            select[:, col] = (rows >> k) == 2 * i + 1
            member[col, :] = (rows >> k) == 2 * i
            level[col] = k + 1
            col += 1
    return np.concatenate([select, select], 0), member, level


class Sems:
    def __init__(self, send, recv):
        self.send, self.recv, self.used = send, recv, 0

    def take(self):
        at = self.used
        self.used += 1
        return (None if self.send is None else (self.send.at[at], self.recv.at[at]))


def kernel(cfg, *refs):
    nz, ny, nx, ly, lz = cfg
    nl = 1 + ly + lz
    ch = T // ny
    nq = nx // 2
    rz = 512 // nz
    ry = rz // ny
    names = (
        "in0", "in1", "in2", "in3", "in4", "in5", "in6", "in7", "in8", "in9", "o_out", "o_dq", "o_dk", "o_dv", "o_dh", "o_dw",
        "part", "rX", "kv", "kvf", "pk", "S", "rB", "tY", "TT", "rC", "UZ", "U", "sQ", "lw2", "G", "Gf", "pG", "GS",
        "rD", "GZ", "rC2", "R", "adj", "oacc", "dq", "dk", "dv", "gl", "sig", "lwb", "gpA", "dws", "rDW", "dw0a", "rd0a", "dw1a", "rd1a",
        "dw0b", "rd0b", "dw1b", "rd1b",  "hid", "w", "q", "k", "v", "g", "dst", "sel", "mem", "lev",
        "scs", "gms", "hidp", "send", "recv", "load",
    )
    r = dict(zip(names, refs, strict=True))
    hid, w, q, k, v, g = (r[n] for n in ("hid", "w", "q", "k", "v", "g"))
    sems = Sems(r["send"], r["recv"])

    s = lax.axis_index("seq")
    x = lax.axis_index("head")
    c = s % 2
    y = (s // 2) % ny
    z = s // (2 * ny)

    def dev(zz, yy, cc, xx):
        return (zz * (2 * ny) + yy * 2 + cc, xx)

    def rc(src, dst, sem, to):
        return pltpu.make_async_remote_copy(
            src_ref=src, dst_ref=dst, send_sem=sem[0], recv_sem=sem[1], device_id=to,
            device_id_type=pl.DeviceIdType.MESH,
        )

    partner = dev(z, y, 1 - c, x)
    y_order = sorted(range(1, ny), key=lambda d: -min(d, ny - d))
    z_order = sorted(range(1, nz), key=lambda d: -min(d, nz - d))
    x_order = sorted(range(1, nx), key=lambda d: -min(d, nx - d))
    pending = []

    def arrive(ref, sem):
        rc(ref, ref, sem, partner).wait_recv()

    def leave(ref, sem, cond=None):
        pending.append((cond, rc(ref, ref, sem, partner)))

    def chunks(n):
        return r["rB"].at[pl.ds(0, n)]

    def when(cond, action):
        if cond is None:
            action()
        else:
            pl.when(cond)(action)

    def bit(value, j):
        return (value // (1 << j)) % 2

    def rows(at, count):
        return pl.ds(pl.multiple_of(at * count, count), count)

    arrays = ("hid", "w", "q", "k", "v", "g", "dst", "sel", "mem", "lev")
    loads = {n: pltpu.make_async_copy(r[f"in{i}"], r[n], r["load"].at[i]) for i, n in enumerate(arrays)}

    def loaded(*wanted):
        for n in wanted:
            loads[n].wait()

    U, G, pG = r["U"], r["G"], r["pG"]
    barrier = pltpu.get_barrier_semaphore()
    peers = [partner]
    peers += [dev(z, y, c, (x + d) % nx) for d in x_order]
    for t in (c, 1 - c):
        peers += [dev(z, (y + d) % ny, t, x) for d in y_order]
        peers += [dev((z + d) % nz, y, t, x) for d in z_order]
    for peer in peers:
        pl.semaphore_signal(barrier, inc=1, device_id=peer, device_id_type=pl.DeviceIdType.MESH)
    for n in ("k", "v", "hid", "w", "q", "g", "mem", "sel", "lev", "dst"):
        loads[n].start()
    for level in range(nl):
        U[level] = jnp.zeros((512, 128), BF16)

    lane = lax.broadcasted_iota(jnp.int32, (1, 128), 1)
    low = lane < DK

    def pair_rows(full):
        return jnp.concatenate([full[:DK, :128], full[DK:, 128:]], 0)

    def spread_pair(block):
        zero = jnp.zeros((DK, 128), block.dtype)
        left = jnp.concatenate([block[:DK], zero], 0)
        right = jnp.concatenate([zero, block[DK:]], 0)
        return jnp.concatenate([left, right], 1)

    def l128(p):
        return pl.ds(pl.multiple_of(p * 128, 128), 128)

    def l256(p):
        return pl.ds(pl.multiple_of(p * 256, 256), 256)

    loaded("k", "v")
    for p in range(4):
        full = dot(k[:, l128(p)], v[:, l256(p)], 0, 0)
        state = pair_rows(full)
        r["kvf"][pl.ds(p * 128, 128), :] = state
        r["kv"][pl.ds(p * 128, 128), :] = state.astype(BF16)
    loaded("hid", "w")
    for j in range(nx):
        r["part"][j] = mm(hid[...], w[:, pl.ds(j * 128, 128)])

    pl.semaphore_wait(barrier, len(peers))

    a_copy = rc(r["kv"], r["pk"], sems.take(), partner)
    a_copy.start()
    pending.append((None, a_copy))
    x_sem = sems.take()
    for d in x_order:
        to = (x + d) % nx
        rc(r["part"].at[to], r["rX"].at[x], x_sem, dev(z, y, c, to)).start()
    leave(r["part"].at[0:nx - 1], x_sem)

    src = lax.broadcasted_iota(jnp.int32, (512, 512), 0)
    col = lax.broadcasted_iota(jnp.int32, (512, 512), 1)
    wanted = ((col // ry) % nz) * rz + (col // (nz * ry)) * ry + col % ry
    r["hidp"][...] = mm(hid[...], jnp.where(src == wanted, 1.0, 0.0).astype(BF16)).astype(BF16)

    a_copy.wait_recv()
    half = rows(c, T)
    mine = r["kvf"][half, :] + r["pk"][half, :].astype(F32)
    r["S"][...] = mine.astype(BF16)
    U[0] = (r["pk"][...].astype(F32) * c.astype(F32)).astype(BF16)
    b_sem = sems.take()
    for d in y_order:
        to = (y + d) % ny
        rc(r["S"].at[rows(to, ch)], r["rB"].at[y], b_sem, dev(z, to, c, x)).start()
    leave(chunks(ny - 1), b_sem)
    r["rB"][y] = r["S"][rows(y, ch), :]

    loaded("q", "g", "mem", "sel", "lev")
    head_row = lax.broadcasted_iota(jnp.int32, (128, 384), 0)

    def level_columns(head):
        return jnp.where(head_row == head * LEVELS + r["lev"][...], 1.0, 0.0).astype(BF16)

    def split_in_two(value):
        upper_part = value.astype(BF16)
        return jnp.concatenate([upper_part, (value - upper_part.astype(F32)).astype(BF16)], 1)

    def scores(p, carry):
        q2 = q[:, l128(p)]
        k2 = k[:, l128(p)]
        member = r["mem"][...]
        gl = r["gl"][...]
        for i in range(2):
            mask = low if i == 0 else jnp.logical_not(low)
            qh = jnp.where(mask, q2, jnp.zeros_like(q2))
            at = pl.ds(pl.multiple_of(p * 256 + i * 128, 128), 128)
            sc = dot(qh, k2, 1, 1)
            gm = dot(g[:, at], v[:, at], 1, 1)
            sc = jnp.concatenate([sc[:128, :128], sc[128:, 128:], sc[128:, :128]], 0)
            gm = jnp.concatenate([gm[:128, :128], gm[128:, 128:], gm[128:, :128]], 0)
            r["scs"][2 * p + i] = sc
            r["gms"][2 * p + i] = gm
            table = level_columns(2 * p + i)
            prod = split_in_two(sc * gm)
            near = dot(prod[:256], jnp.concatenate([member, member], 1), 1, 1)
            near = near.astype(BF16) * r["sel"][...]
            gl = gl + dot(near, table[:, :256], 1, 1)
            far = dot(prod[256:], jnp.concatenate([table[:, 256:], table[:, 256:]], 1), 1, 1)
            gl = gl + jnp.concatenate([jnp.zeros((128, 128), F32), far], 0)
        r["gl"][...] = gl
        return carry

    r["gl"][...] = jnp.zeros((T, 128), F32)
    lax.fori_loop(0, 4, scores, 0)

    arrive(chunks(ny - 1), b_sem)
    sums = [r["rB"][i].astype(F32) for i in range(ny)]
    for j in range(1, ly):
        sums = [sums[2 * i] + sums[2 * i + 1] for i in range(len(sums) // 2)]
        for i, value in enumerate(sums):
            r["tY"][j, i] = value.astype(BF16)
    r["TT"][...] = (sums[0] + sums[1]).astype(BF16)
    c_sem = sems.take()
    for d in range(nz - 1, 0, -1):
        to = (z + d) % nz
        cp = rc(r["TT"], r["rC"].at[z], c_sem, dev(to, y, c, x))
        when(z + d < nz, cp.start)
    for at in range(nz - 1):
        leave(r["rC"].at[0:nz - 1 - at], c_sem, z == at)

    def y_source(level, target):
        at = target // (1 << level) - 1
        at = (at + ny) % ny
        return r["rB"].at[at] if level == 0 else r["tY"].at[level, at]

    slot = c * ny + y
    d_sems = [sems.take() for _ in range(ly + lz)]
    for level in range(ly):
        for d in y_order:
            to = (y + d) % ny
            cp = rc(
                y_source(level, to), U.at[1 + level, rows(slot, ch)], d_sems[level], dev(z, to, c, x)
            )
            when(bit(to, level) == 1, cp.start)
        for own in range(2):
            if ny // 2 - own:
                leave(chunks(ny // 2 - own), d_sems[level], bit(y, level) == own)

        @pl.when(bit(y, level) == 1)
        def _():
            U[1 + level, rows(slot, ch), :] = y_source(level, y)[...]

    arrive(r["rX"].at[0:nx - 1], x_sem)
    r["rX"][x] = r["part"][x]
    projected = r["rX"][0]
    for j in range(1, nx):
        projected = projected + r["rX"][j]
    weights = jnp.maximum(projected, 0.0) + jnp.log1p(jnp.exp(-jnp.abs(projected)))
    upper_part = weights.astype(BF16)
    rest = (weights - upper_part.astype(F32)).astype(BF16)
    r["lwb"][...] = jnp.concatenate([upper_part, rest], 1)
    r["sig"][...] = jax.nn.sigmoid(projected)

    row_id = lax.broadcasted_iota(jnp.int32, (128, nl * 128), 0)
    col_id = lax.broadcasted_iota(jnp.int32, (128, nl * 128), 1)
    col_level = BASE + col_id // 128
    col_head = (col_id % 128) // DK

    def upper_table(p):
        return jnp.where(row_id == (2 * p + col_head) * LEVELS + col_level, 1.0, 0.0).astype(BF16)

    def grad_states(p, carry):
        table = upper_table(p)
        wide = mm(r["lwb"][...], jnp.concatenate([table, table], 0))
        r["lw2"][p] = wide.astype(BF16)
        q2 = q[:, l128(p)].astype(F32)
        gg = g[:, l256(p)]
        for m in range(nl):
            scaled = (wide[:, m * 128:(m + 1) * 128] * q2).astype(BF16)
            r["sQ"][p, :, m * 128:(m + 1) * 128] = scaled
            state = pair_rows(dot(scaled, gg, 0, 0))
            r["Gf"][m, rows(p, 128), :] = state
            G[m, rows(p, 128), :] = state.astype(BF16)
        return carry

    lax.fori_loop(0, 4, grad_states, 0)
    ga = rc(G.at[0], pG.at[0], sems.take(), partner)
    ga.start()
    pending.append((None, ga))
    other = rows(1 - c, T)
    gb = rc(G.at[1:nl, other], pG.at[1:nl, other], sems.take(), partner)
    gb.start()
    pending.append((None, gb))

    def local_pair(p, carry):
        q2 = q[:, l128(p)]
        k2 = k[:, l128(p)]
        select = r["sel"][...]
        member = r["mem"][...]
        dq2 = jnp.zeros((T, 128), F32)
        dk2 = jnp.zeros((T, 128), F32)
        zero = jnp.zeros((128, 128), BF16)
        for i in range(2):
            mask = low if i == 0 else jnp.logical_not(low)
            qh = jnp.where(mask, q2, jnp.zeros_like(q2))
            kh = jnp.where(mask, k2, jnp.zeros_like(k2))
            at = pl.ds(pl.multiple_of(p * 256 + i * 128, 128), 128)
            vh = v[:, at]
            gh = g[:, at]
            table = level_columns(2 * p + i)
            wide = mm(r["lwb"][...], jnp.concatenate([table, table], 0))
            chosen = wide[:, :256].astype(BF16) * select
            spread = mm(chosen, member)
            far = wide[128:, 256:]
            both = jnp.concatenate([spread, far], 0)
            mixed = (r["scs"][2 * p + i] * both).astype(BF16)
            gs = (r["gms"][2 * p + i] * both).astype(BF16)

            def square(block):
                top = jnp.concatenate([block[:128], zero], 1)
                return jnp.concatenate([top, jnp.concatenate([block[256:], block[128:256]], 1)], 0)

            mixed = square(mixed)
            gs = square(gs)
            r["oacc"][:, at] = mm(mixed, vh)
            r["dv"][:, at] = dot(mixed, gh, 0, 0)
            dq2 = dq2 + mm(gs, kh)
            dk2 = dk2 + dot(gs, qh, 0, 0)
        r["dq"][:, l128(p)] = dq2
        r["dk"][:, l128(p)] = dk2
        return carry

    lax.fori_loop(0, 1, local_pair, 0)

    for at in range(1, nz):
        when(z == at, rc(r["rC"].at[0:at], r["rC"].at[0:at], c_sem, partner).wait_recv)
    for level in range(lz):
        @pl.when(bit(z, level) == 1)
        def _():
            start = (z // (1 << level) - 1) * (1 << level)
            value = r["rC"][start].astype(F32)
            for i in range(1, 1 << level):
                value = value + r["rC"][start + i].astype(F32)
            r["UZ"][level] = value.astype(BF16)
            for d in y_order:
                to = (y + d) % ny
                rc(
                    r["UZ"].at[level], U.at[1 + ly + level, rows(slot, ch)], d_sems[ly + level], dev(z, to, c, x)
                ).start()
            U[1 + ly + level, rows(slot, ch), :] = r["UZ"][level]
        leave(chunks(ny - 1), d_sems[ly + level], bit(z, level) == 1)

    def shared(first, last):
        for level in range(first, last):
            own_bit = bit(y, level) if level < ly else bit(z, level - ly)
            when(own_bit == 1, rc(chunks(ny - 1), chunks(ny - 1), d_sems[level], partner).wait_recv)
        part = U.at[1 + first:1 + last, half]
        cp = rc(part, part, sems.take(), partner)
        cp.start()
        pending.append((None, cp))
        return cp

    share_y = shared(0, ly)

    gb.wait_recv()
    for level in range(ly + lz):
        both = r["Gf"][1 + level, half, :] + pG[1 + level, half, :].astype(F32)
        r["GS"][level] = both.astype(BF16)
    e_sems = [sems.take() for _ in range(ly + lz)]
    for level in range(ly + lz):
        own_bit = bit(y, level) if level < ly else bit(z, level - ly)
        leave(chunks(ny - 1), e_sems[level], own_bit == 1)

        @pl.when(own_bit == 1)
        def _():
            for d in y_order:
                to = (y + d) % ny
                rc(
                    r["GS"].at[level, rows(to, ch)], r["rD"].at[y, level], e_sems[level], dev(z, to, c, x)
                ).start()
            r["rD"][y, level] = r["GS"][level, rows(y, ch), :]

    lax.fori_loop(1, 4, local_pair, 0)

    def states_of(p, first, last):
        return jnp.concatenate([spread_pair(U[m, rows(p, 128), :]) for m in range(first, last)], 0)

    def add_levels(p, back, first, last):
        count = last - first
        q2 = q[:, l128(p)].astype(F32)
        terms = [split_in_two(back[:, m * 128:(m + 1) * 128] * q2) for m in range(count)]
        out_row = lax.broadcasted_iota(jnp.int32, (count * 256, 128), 0)
        out_col = lax.broadcasted_iota(jnp.int32, (count * 256, 128), 1)
        table = jnp.where(
            out_col == (2 * p + (out_row % 128) // DK) * LEVELS + BASE + first + out_row // 256, 1.0, 0.0
        ).astype(BF16)
        r["gl"][...] += mm(jnp.concatenate(terms, 1), table)

    def add_states(p, back, wide, first, last):
        columns = slice(first * 128, last * 128)
        out = r["oacc"][:, l256(p)] + mm(r["sQ"][p, :, columns], wide)
        dq2 = r["dq"][:, l128(p)]
        for m in range(last - first):
            at = slice((first + m) * 128, (first + m + 1) * 128)
            dq2 = dq2 + r["lw2"][p, :, at].astype(F32) * back[:, m * 128:(m + 1) * 128]
        return out, dq2

    def near_levels(p, carry):
        wide = states_of(p, 0, 1 + ly)
        back = dot(g[:, l256(p)], wide, 1, 1)
        add_levels(p, back, 0, 1 + ly)
        out, dq2 = add_states(p, back, wide, 0, 1 + ly)
        r["oacc"][:, l256(p)] = out
        r["dq"][:, l128(p)] = dq2
        return carry

    def far_levels(p, carry):
        add_levels(p, dot(g[:, l256(p)], states_of(p, 1 + ly, nl), 1, 1), 1 + ly, nl)
        return carry

    def far_states(p, carry):
        wide = states_of(p, 1 + ly, nl)
        out, dq2 = add_states(p, dot(g[:, l256(p)], wide, 1, 1), wide, 1 + ly, nl)
        r["o_out"][:, l256(p)] = out.astype(BF16)
        r["o_dq"][:, l128(p)] = dq2.astype(BF16)
        return carry

    share_y.wait_recv()
    lax.fori_loop(0, 4, near_levels, 0)
    share_z = shared(ly, ly + lz)
    share_z.wait_recv()
    lax.fori_loop(0, 4, far_levels, 0)
    gp = (r["gl"][...] * r["sig"][...]).astype(BF16)
    r["gpA"][x] = gp
    g_sem = sems.take()
    for d in x_order:
        to = (x + d) % nx
        rc(r["gpA"].at[x], r["gpA"].at[x], g_sem, dev(z, y, c, to)).start()
    leave(r["gpA"].at[0:nx - 1], g_sem)

    lax.fori_loop(0, 4, far_states, 0)

    for level in range(ly + lz):
        if level >= ly:
            when(bit(z, level - ly) == 1, rc(chunks(ny - 1), chunks(ny - 1), e_sems[level], partner).wait_recv)
            continue
        for own in range(2):
            n = ny // 2 - own
            if n:
                when(bit(y, level) == own, rc(chunks(n), chunks(n), e_sems[level], partner).wait_recv)
    for level in range(lz):
        @pl.when(bit(z, level) == 1)
        def _():
            value = r["rD"][0, ly + level].astype(F32)
            for i in range(1, ny):
                value = value + r["rD"][i, ly + level].astype(F32)
            r["GZ"][level] = value.astype(BF16)
    f_sem = sems.take()
    for d in range(nz - 1, 0, -1):
        to = (z + nz - d) % nz
        top = 0
        for level in range(lz):
            apart = z // (1 << level) - to // (1 << level)
            top = top + (apart + nz - 1) // nz
        at = (top + lz - 1) % lz
        cp = rc(r["GZ"].at[at], r["rC2"].at[z], f_sem, dev(to, y, c, x))
        when(z >= d, cp.start)
    for at in range(1, nz):
        leave(r["rC2"].at[0:at], f_sem, z == at)

    arrive(r["gpA"].at[0:nx - 1], g_sem)
    def left(j):
        return hid[...] if j % 2 == 0 else r["hidp"][...]

    for j in range(nq):
        r["dws"][j] = dot(left(j), r["gpA"][(1 - c) * nq + j], 0, 0).astype(BF16)
    w_copy = rc(r["dws"], r["rDW"], sems.take(), partner)
    w_copy.start()
    pending.append((None, w_copy))
    own_dw = [dot(left(j), r["gpA"][c * nq + j], 0, 0) for j in range(nq)]

    d_hidden = dot(r["gpA"][0], w[:, 0:128], 1, 1)
    for j in range(1, nx):
        d_hidden = d_hidden + dot(r["gpA"][j], w[:, j * 128:(j + 1) * 128], 1, 1)
    r["o_dh"][...] = d_hidden.astype(BF16)

    def along(axis, d):
        return (dev((z + d) % nz, y, c, x), (z + d) % nz) if axis == 0 else (dev(z, (y + d) % ny, c, x), (y + d) % ny)

    here = (z, y)
    orders = (z_order, y_order)
    counts = (nz, ny)
    w_copy.wait_recv()
    first_sems = [sems.take() for _ in range(nq)]
    for j in range(nq):
        both = own_dw[j] + r["rDW"][j].astype(F32)
        axis = j % 2
        size = 512 // counts[axis]
        for i in range(counts[axis]):
            r[f"dw{j}a"][i] = both[i * size:(i + 1) * size].astype(BF16)
        for d in orders[axis]:
            device, to = along(axis, d)
            rc(r[f"dw{j}a"].at[to], r[f"rd{j}a"].at[here[axis]], first_sems[j], device).start()
        leave(r[f"dw{j}a"].at[0:counts[axis] - 1], first_sems[j])
        r[f"rd{j}a"][here[axis]] = r[f"dw{j}a"][here[axis]]

    for at in range(nz - 1):
        part = r["rC2"].at[0:nz - 1 - at]
        when(z == at, rc(part, part, f_sem, partner).wait_recv)
    r["rC2"][z] = jnp.zeros((ch, 128), BF16)
    for i in range(nz):
        @pl.when(i < z)
        def _():
            r["rC2"][i] = jnp.zeros((ch, 128), BF16)
    from_z = r["rC2"][0].astype(F32)
    for i in range(1, nz):
        from_z = from_z + r["rC2"][i].astype(F32)
    for i in range(ny):
        value = from_z
        for later in range(i + 1, ny):
            value = value + r["rD"][later, (i ^ later).bit_length() - 1].astype(F32)
        r["R"][i] = value.astype(BF16)
    h_sem = sems.take()
    for d in y_order:
        to = (y + d) % ny
        rc(r["R"].at[to], r["adj"].at[rows(slot, ch)], h_sem, dev(z, to, c, x)).start()
    leave(chunks(ny - 1), h_sem)
    r["adj"][rows(slot, ch), :] = r["R"][y]

    second_sems = [sems.take() for _ in range(nq)]
    keep = ry // 2
    for j in range(nq):
        axis = j % 2
        arrive(r[f"rd{j}a"].at[0:counts[axis] - 1], first_sems[j])
        value = r[f"rd{j}a"][0].astype(F32)
        for i in range(1, counts[axis]):
            value = value + r[f"rd{j}a"][i].astype(F32)
        axis = 1 - axis
        count = counts[axis]
        for i in range(count):
            for t in range(2):
                r[f"dw{j}b"][2 * i + t] = value[i * ry + t * keep:i * ry + (t + 1) * keep]
        place = r[f"rd{j}b"].at[c * count + here[axis]]
        for d in [*orders[axis], 0]:
            spot = (here[axis] + d) % count
            for t in (1 - c, c)[:2 if d else 1]:
                device = dev(spot, y, t, x) if axis == 0 else dev(z, spot, t, x)
                rc(r[f"dw{j}b"].at[2 * spot + t], place, second_sems[j], device).start()
        leave(r[f"dw{j}b"].at[0:2 * count - 1], second_sems[j])
        r[f"rd{j}b"][c * count + here[axis]] = r[f"dw{j}b"][2 * here[axis] + c]

    arrive(chunks(ny - 1), h_sem)
    adj_share = rc(r["adj"].at[half], r["adj"].at[half], sems.take(), partner)
    adj_share.start()
    pending.append((None, adj_share))

    loaded("dst")
    adj_share.wait_recv()
    ga.wait_recv()
    first = (1 - c).astype(F32)

    def finish(p, carry):
        at = rows(p, 128)
        total = r["dst"][at, :] + r["adj"][at, :].astype(F32) + pG[0, at, :].astype(F32) * first
        wide = spread_pair(total.astype(BF16))
        dk2 = r["dk"][:, l128(p)] + dot(v[:, l256(p)], wide, 1, 1)
        r["o_dk"][:, l128(p)] = dk2.astype(BF16)
        dv2 = r["dv"][:, l256(p)] + mm(k[:, l128(p)], wide)
        r["o_dv"][:, l256(p)] = dv2.astype(BF16)
        return carry

    lax.fori_loop(0, 4, finish, 0)

    for j in range(nq):
        count = counts[1 - j % 2]
        arrive(r[f"rd{j}b"].at[0:2 * count - 1], second_sems[j])
        for t in range(2):
            value = r[f"rd{j}b"][t * count]
            for i in range(1, count):
                value = value + r[f"rd{j}b"][t * count + i]
            r["o_dw"][:, (t * nq + j) * 128:(t * nq + j + 1) * 128] = value

    assert sems.used == r["send"].shape[0]
    for cond, cp in pending:
        if cond is None:
            cp.wait_send()
        else:
            @pl.when(cond)
            def _():
                cp.wait_send()


def write_out(*refs):
    count = len(refs) // 2
    sem = refs[-1]
    copies = [pltpu.make_async_copy(refs[i], refs[count + i], sem.at[i]) for i in range(count)]
    for cp in copies:
        cp.start()
    for cp in copies:
        cp.wait()


def build(mesh, nz, ny):
    nx = mesh.shape["head"]
    ly, lz = ny.bit_length() - 1, nz.bit_length() - 1
    nl = 1 + ly + lz
    ch = T // ny
    nq = nx // 2
    rz = 512 // nz
    ry = rz // ny
    n_sem = 13 + 2 * (ly + lz) + 2 * nq
    select, member, level = segment_tables()
    levels_of = np.concatenate([level, np.full((128,), 8, np.int32)])[None]
    vm = pltpu.VMEM
    wide = nx * 128
    scratch = [
        vm((nx, T, 128), F32), vm((nx, T, 128), F32),
        vm((512, 128), BF16), vm((512, 128), F32), vm((512, 128), BF16), vm((T, 128), BF16),
        vm((ny, ch, 128), BF16), vm((max(ly, 1), max(ny // 2, 1), ch, 128), BF16), vm((ch, 128), BF16),
        vm((nz, ch, 128), BF16), vm((lz, ch, 128), BF16), vm((nl, 512, 128), BF16),
        vm((4, T, nl * 128), BF16), vm((4, T, nl * 128), BF16),
        vm((nl, 512, 128), BF16), vm((nl, 512, 128), F32), vm((nl, 512, 128), BF16), vm((nl - 1, T, 128), BF16),
        vm((ny, nl - 1, ch, 128), BF16), vm((lz, ch, 128), BF16), vm((nz, ch, 128), BF16),
        vm((ny, ch, 128), BF16), vm((512, 128), BF16),
        vm((T, 1024), F32), vm((T, 512), F32), vm((T, 512), F32), vm((T, 1024), F32),
        vm((T, 128), F32), vm((T, 128), F32), vm((T, 256), BF16),
        vm((nx, T, 128), BF16),
        vm((nq, 512, 128), BF16), vm((nq, 512, 128), BF16),
        vm((nz, rz, 128), BF16), vm((nz, rz, 128), BF16),
        vm((ny, 512 // ny, 128), BF16), vm((ny, 512 // ny, 128), BF16),
        vm((2 * ny, ry // 2, 128), F32), vm((2 * ny, ry // 2, 128), F32),
        vm((2 * nz, ry // 2, 128), F32), vm((2 * nz, ry // 2, 128), F32),
        vm((T, 512), BF16), vm((512, wide), BF16), vm((T, 512), BF16), vm((T, 512), BF16),
        vm((T, 1024), BF16), vm((T, 1024), BF16), vm((512, 128), F32),
        vm((T, 256), BF16), vm((T, 128), BF16), vm((1, 384), jnp.int32),
        vm((8, 384, 128), F32), vm((8, 384, 128), F32), vm((T, 512), BF16),
        pltpu.SemaphoreType.DMA((n_sem,)), pltpu.SemaphoreType.DMA((n_sem,)), pltpu.SemaphoreType.DMA((10,)),
    ]

    results = [
        jax.ShapeDtypeStruct((T, 1024), BF16),
        jax.ShapeDtypeStruct((T, 512), BF16),
        jax.ShapeDtypeStruct((T, 512), BF16),
        jax.ShapeDtypeStruct((T, 1024), BF16),
        jax.ShapeDtypeStruct((T, 512), BF16),
        jax.ShapeDtypeStruct((ry // 2, wide), F32),
    ]

    def step(hidden, w, q, k, v, g, d_state):
        operands = (
            hidden, w, q, k, v, g, d_state.reshape(512, DV),
            jnp.asarray(select, BF16), jnp.asarray(member, BF16), jnp.asarray(levels_of),
        )
        outs = pl.pallas_call(
            functools.partial(kernel, (nz, ny, nx, ly, lz)),
            out_shape=[pltpu.VMEM(a.shape, a.dtype) for a in results],
            in_specs=[pl.BlockSpec(memory_space=pltpu.HBM)] * 10,
            out_specs=[pl.BlockSpec(memory_space=pltpu.VMEM)] * 6,
            scratch_shapes=scratch,
            compiler_params=pltpu.CompilerParams(
                collective_id=0, has_side_effects=True, vmem_limit_bytes=36 * 1024 * 1024
            ),
        )(
            *(pltpu.with_memory_space_constraint(a, pltpu.HBM) for a in operands)
        )
        return pl.pallas_call(
            write_out,
            out_shape=results,
            in_specs=[pl.BlockSpec(memory_space=pltpu.VMEM)] * 6,
            out_specs=[pl.BlockSpec(memory_space=pltpu.HBM)] * 6,
            scratch_shapes=[pltpu.SemaphoreType.DMA((6,))],
            compiler_params=pltpu.CompilerParams(vmem_limit_bytes=8 * 1024 * 1024),
        )(*outs)

    both = P("seq", "head")
    return jax.shard_map(
        step,
        mesh=mesh,
        in_specs=(both, P("head", None), both, both, both, both, P("head", None, None)),
        out_specs=(both, both, both, both, both, P(("head", "seq"), None)),
        check_vma=False,
    )


def solution(mesh):
    return build(mesh, 8, 8)
```

```python
import functools

import jax
import jax.numpy as jnp
import numpy as np
from jax import lax
from jax.experimental import pallas as pl
from jax.experimental.pallas import tpu as pltpu
from jax.sharding import PartitionSpec as P

DK = 64
DV = 128
LEVELS = 16
BASE = 9
T = 256
F32 = jnp.float32
BF16 = jnp.bfloat16


def dot(a, b, da, db):
    return lax.dot_general(a, b, (((da,), (db,)), ((), ())), preferred_element_type=F32)


def mm(a, b):
    return dot(a, b, 1, 0)


def segment_tables():
    select = np.zeros((128, 256), np.float32)
    member = np.zeros((256, 128), np.float32)
    level = np.full((256,), 99, np.int32)
    level[:128] = 0
    rows = np.arange(128)
    select[rows, rows] = 1.0
    member[rows, rows] = 1.0
    col = 128
    for k in range(7):
        for i in range(64 >> k):
            select[:, col] = (rows >> k) == 2 * i + 1
            member[col, :] = (rows >> k) == 2 * i
            level[col] = k + 1
            col += 1
    return np.concatenate([select, select], 0), member, level


class Sems:
    def __init__(self, send, recv):
        self.send, self.recv, self.used = send, recv, 0

    def take(self):
        at = self.used
        self.used += 1
        return (None if self.send is None else (self.send.at[at], self.recv.at[at]))


def kernel(cfg, *refs):
    nz, ny, nx, ly, lz = cfg
    nl = 1 + ly + lz
    ch = T // ny
    nq = nx // 2
    rz = 512 // nz
    ry = rz // ny
    names = (
        "in0", "in1", "in2", "in3", "in4", "in5", "in6", "in7", "in8", "in9", "o_out", "o_dq", "o_dk", "o_dv", "o_dh", "o_dw",
        "part", "rX", "kv", "kvf", "pk", "S", "rB", "tY", "TT", "rC", "UZ", "U", "sQ", "lw2", "G", "Gf", "pG", "GS",
        "rD", "GZ", "rC2", "R", "adj", "oacc", "dq", "dk", "dv", "gl", "sig", "lwb", "gpA", "dws", "rDW", "dw0a", "rd0a", "dw1a", "rd1a",
        "dw0b", "rd0b", "dw1b", "rd1b",  "hid", "w", "q", "k", "v", "g", "dst", "sel", "mem", "lev",
        "scs", "gms", "hidp", "swap", "gpL", "gpH", "send", "recv", "load",
    )
    r = dict(zip(names, refs, strict=True))
    hid, w, q, k, v, g = (r[n] for n in ("hid", "w", "q", "k", "v", "g"))
    sems = Sems(r["send"], r["recv"])

    s = lax.axis_index("seq")
    x = lax.axis_index("head")
    c = s % 2
    y = (s // 2) % ny
    z = s // (2 * ny)

    def dev(zz, yy, cc, xx):
        return (zz * (2 * ny) + yy * 2 + cc, xx)

    def rc(src, dst, sem, to):
        return pltpu.make_async_remote_copy(
            src_ref=src, dst_ref=dst, send_sem=sem[0], recv_sem=sem[1], device_id=to,
            device_id_type=pl.DeviceIdType.MESH,
        )

    partner = dev(z, y, 1 - c, x)
    y_order = sorted(range(1, ny), key=lambda d: -min(d, ny - d))
    z_order = sorted(range(1, nz), key=lambda d: -min(d, nz - d))
    x_order = sorted(range(1, nx), key=lambda d: -min(d, nx - d))
    pending = []

    def arrive(ref, sem):
        rc(ref, ref, sem, partner).wait_recv()

    def leave(ref, sem, cond=None):
        pending.append((cond, rc(ref, ref, sem, partner)))

    def chunks(n):
        return r["rB"].at[pl.ds(0, n)]

    def when(cond, action):
        if cond is None:
            action()
        else:
            pl.when(cond)(action)

    def bit(value, j):
        return (value // (1 << j)) % 2

    def rows(at, count):
        return pl.ds(pl.multiple_of(at * count, count), count)

    arrays = ("hid", "w", "q", "k", "v", "g", "dst", "sel", "mem", "lev")
    loads = {n: pltpu.make_async_copy(r[f"in{i}"], r[n], r["load"].at[i]) for i, n in enumerate(arrays)}

    def loaded(*wanted):
        for n in wanted:
            loads[n].wait()

    U, G, pG = r["U"], r["G"], r["pG"]
    barrier = pltpu.get_barrier_semaphore()
    peers = [partner]
    peers += [dev(z, y, c, (x + d) % nx) for d in x_order]
    for t in (c, 1 - c):
        peers += [dev(z, (y + d) % ny, t, x) for d in y_order]
        peers += [dev((z + d) % nz, y, t, x) for d in z_order]
    for peer in peers:
        pl.semaphore_signal(barrier, inc=1, device_id=peer, device_id_type=pl.DeviceIdType.MESH)
    for n in ("k", "v", "hid", "w", "q", "g", "mem", "sel", "lev", "dst"):
        loads[n].start()
    for level in range(nl):
        U[level] = jnp.zeros((512, 128), BF16)

    lane = lax.broadcasted_iota(jnp.int32, (1, 128), 1)
    low = lane < DK

    def pair_rows(full):
        return jnp.concatenate([full[:DK, :128], full[DK:, 128:]], 0)

    def spread_pair(block):
        zero = jnp.zeros((DK, 128), block.dtype)
        left = jnp.concatenate([block[:DK], zero], 0)
        right = jnp.concatenate([zero, block[DK:]], 0)
        return jnp.concatenate([left, right], 1)

    def l128(p):
        return pl.ds(pl.multiple_of(p * 128, 128), 128)

    def l256(p):
        return pl.ds(pl.multiple_of(p * 256, 256), 256)

    loaded("k", "v")
    for p in range(4):
        full = dot(k[:, l128(p)], v[:, l256(p)], 0, 0)
        state = pair_rows(full)
        r["kvf"][pl.ds(p * 128, 128), :] = state
        r["kv"][pl.ds(p * 128, 128), :] = state.astype(BF16)
    loaded("hid", "w")
    for j in range(nx):
        r["part"][j] = mm(hid[...], w[:, pl.ds(j * 128, 128)])

    pl.semaphore_wait(barrier, len(peers))

    a_copy = rc(r["kv"], r["pk"], sems.take(), partner)
    a_copy.start()
    pending.append((None, a_copy))
    x_sem = sems.take()
    for d in x_order:
        to = (x + d) % nx
        rc(r["part"].at[to], r["rX"].at[x], x_sem, dev(z, y, c, to)).start()
    leave(r["part"].at[0:nx - 1], x_sem)

    src = lax.broadcasted_iota(jnp.int32, (512, 512), 0)
    col = lax.broadcasted_iota(jnp.int32, (512, 512), 1)
    wanted = ((col // ry) % nz) * rz + (col // (nz * ry)) * ry + col % ry
    r["hidp"][...] = mm(hid[...], jnp.where(src == wanted, 1.0, 0.0).astype(BF16)).astype(BF16)

    src = lax.broadcasted_iota(jnp.int32, (T, T), 0)
    col = lax.broadcasted_iota(jnp.int32, (T, T), 1)
    level = src % LEVELS
    packed = (level // 8) * 128 + (src // 128) * 64 + ((src % 128) // LEVELS) * 8 + level % 8
    r["swap"][...] = jnp.where(col == packed, 1.0, 0.0).astype(BF16)

    a_copy.wait_recv()
    half = rows(c, T)
    mine = r["kvf"][half, :] + r["pk"][half, :].astype(F32)
    r["S"][...] = mine.astype(BF16)
    U[0] = (r["pk"][...].astype(F32) * c.astype(F32)).astype(BF16)
    b_sem = sems.take()
    for d in y_order:
        to = (y + d) % ny
        rc(r["S"].at[rows(to, ch)], r["rB"].at[y], b_sem, dev(z, to, c, x)).start()
    leave(chunks(ny - 1), b_sem)
    r["rB"][y] = r["S"][rows(y, ch), :]

    loaded("q", "g", "mem", "sel", "lev")
    head_row = lax.broadcasted_iota(jnp.int32, (128, 384), 0)

    def level_columns(head):
        return jnp.where(head_row == head * LEVELS + r["lev"][...], 1.0, 0.0).astype(BF16)

    def split_in_two(value):
        upper_part = value.astype(BF16)
        return jnp.concatenate([upper_part, (value - upper_part.astype(F32)).astype(BF16)], 1)

    def scores(p, carry):
        q2 = q[:, l128(p)]
        k2 = k[:, l128(p)]
        member = r["mem"][...]
        gl = carry
        for i in range(2):
            mask = low if i == 0 else jnp.logical_not(low)
            qh = jnp.where(mask, q2, jnp.zeros_like(q2))
            at = pl.ds(pl.multiple_of(p * 256 + i * 128, 128), 128)
            sc = dot(qh, k2, 1, 1)
            gm = dot(g[:, at], v[:, at], 1, 1)
            sc = jnp.concatenate([sc[:128, :128], sc[128:, 128:], sc[128:, :128]], 0)
            gm = jnp.concatenate([gm[:128, :128], gm[128:, 128:], gm[128:, :128]], 0)
            r["scs"][2 * p + i] = sc
            r["gms"][2 * p + i] = gm
            table = level_columns(2 * p + i)
            prod = split_in_two(sc * gm)
            near = dot(prod[:256], jnp.concatenate([member, member], 1), 1, 1)
            near = near.astype(BF16) * r["sel"][...]
            gl = gl + dot(near, table[:, :256], 1, 1)
            far = dot(prod[256:], jnp.concatenate([table[:, 256:], table[:, 256:]], 1), 1, 1)
            gl = gl + jnp.concatenate([jnp.zeros((128, 128), F32), far], 0)
        return gl

    r["gl"][...] = lax.fori_loop(0, 4, scores, jnp.zeros((T, 128), F32), unroll=4)

    arrive(chunks(ny - 1), b_sem)
    sums = [r["rB"][i].astype(F32) for i in range(ny)]
    for j in range(1, ly):
        sums = [sums[2 * i] + sums[2 * i + 1] for i in range(len(sums) // 2)]
        for i, value in enumerate(sums):
            r["tY"][j, i] = value.astype(BF16)
    r["TT"][...] = (sums[0] + sums[1]).astype(BF16)
    c_sem = sems.take()
    for d in range(nz - 1, 0, -1):
        to = (z + d) % nz
        cp = rc(r["TT"], r["rC"].at[z], c_sem, dev(to, y, c, x))
        when(z + d < nz, cp.start)
    for at in range(nz - 1):
        leave(r["rC"].at[0:nz - 1 - at], c_sem, z == at)

    def y_source(level, target):
        at = target // (1 << level) - 1
        at = (at + ny) % ny
        return r["rB"].at[at] if level == 0 else r["tY"].at[level, at]

    slot = c * ny + y
    d_sems = [sems.take() for _ in range(ly + lz)]
    for level in range(ly):
        for d in y_order:
            to = (y + d) % ny
            cp = rc(
                y_source(level, to), U.at[1 + level, rows(slot, ch)], d_sems[level], dev(z, to, c, x)
            )
            when(bit(to, level) == 1, cp.start)
        for own in range(2):
            if ny // 2 - own:
                leave(chunks(ny // 2 - own), d_sems[level], bit(y, level) == own)

        @pl.when(bit(y, level) == 1)
        def _():
            U[1 + level, rows(slot, ch), :] = y_source(level, y)[...]

    arrive(r["rX"].at[0:nx - 1], x_sem)
    r["rX"][x] = r["part"][x]
    projected = r["rX"][0]
    for j in range(1, nx):
        projected = projected + r["rX"][j]
    weights = jnp.maximum(projected, 0.0) + jnp.log1p(jnp.exp(-jnp.abs(projected)))
    upper_part = weights.astype(BF16)
    rest = (weights - upper_part.astype(F32)).astype(BF16)
    r["lwb"][...] = jnp.concatenate([upper_part, rest], 1)
    r["sig"][...] = jax.nn.sigmoid(projected)

    row_id = lax.broadcasted_iota(jnp.int32, (128, nl * 128), 0)
    col_id = lax.broadcasted_iota(jnp.int32, (128, nl * 128), 1)
    col_level = BASE + col_id // 128
    col_head = (col_id % 128) // DK

    def upper_table(p):
        return jnp.where(row_id == (2 * p + col_head) * LEVELS + col_level, 1.0, 0.0).astype(BF16)

    def grad_states(p, carry):
        table = upper_table(p)
        wide = mm(r["lwb"][...], jnp.concatenate([table, table], 0))
        r["lw2"][p] = wide.astype(BF16)
        q2 = q[:, l128(p)].astype(F32)
        gg = g[:, l256(p)]
        for m in range(nl):
            scaled = (wide[:, m * 128:(m + 1) * 128] * q2).astype(BF16)
            r["sQ"][p, :, m * 128:(m + 1) * 128] = scaled
            state = pair_rows(dot(scaled, gg, 0, 0))
            r["Gf"][m, rows(p, 128), :] = state
            G[m, rows(p, 128), :] = state.astype(BF16)
        return carry

    lax.fori_loop(0, 4, grad_states, 0, unroll=4)
    ga = rc(G.at[0], pG.at[0], sems.take(), partner)
    ga.start()
    pending.append((None, ga))
    other = rows(1 - c, T)
    gb = rc(G.at[1:nl, other], pG.at[1:nl, other], sems.take(), partner)
    gb.start()
    pending.append((None, gb))

    def local_pair(p, carry):
        q2 = q[:, l128(p)]
        k2 = k[:, l128(p)]
        select = r["sel"][...]
        member = r["mem"][...]
        dq2 = jnp.zeros((T, 128), F32)
        dk2 = jnp.zeros((T, 128), F32)
        zero = jnp.zeros((128, 128), BF16)
        for i in range(2):
            mask = low if i == 0 else jnp.logical_not(low)
            qh = jnp.where(mask, q2, jnp.zeros_like(q2))
            kh = jnp.where(mask, k2, jnp.zeros_like(k2))
            at = pl.ds(pl.multiple_of(p * 256 + i * 128, 128), 128)
            vh = v[:, at]
            gh = g[:, at]
            table = level_columns(2 * p + i)
            wide = mm(r["lwb"][...], jnp.concatenate([table, table], 0))
            chosen = wide[:, :256].astype(BF16) * select
            spread = mm(chosen, member)
            far = wide[128:, 256:]
            both = jnp.concatenate([spread, far], 0)
            mixed = (r["scs"][2 * p + i] * both).astype(BF16)
            gs = (r["gms"][2 * p + i] * both).astype(BF16)

            def square(block):
                top = jnp.concatenate([block[:128], zero], 1)
                return jnp.concatenate([top, jnp.concatenate([block[256:], block[128:256]], 1)], 0)

            mixed = square(mixed)
            gs = square(gs)
            r["oacc"][:, at] = mm(mixed, vh)
            r["dv"][:, at] = dot(mixed, gh, 0, 0)
            dq2 = dq2 + mm(gs, kh)
            dk2 = dk2 + dot(gs, qh, 0, 0)
        r["dq"][:, l128(p)] = dq2
        r["dk"][:, l128(p)] = dk2
        return carry

    for at in range(1, nz):
        when(z == at, rc(r["rC"].at[0:at], r["rC"].at[0:at], c_sem, partner).wait_recv)
    for level in range(lz):
        @pl.when(bit(z, level) == 1)
        def _():
            start = (z // (1 << level) - 1) * (1 << level)
            value = r["rC"][start].astype(F32)
            for i in range(1, 1 << level):
                value = value + r["rC"][start + i].astype(F32)
            r["UZ"][level] = value.astype(BF16)
            for d in y_order:
                to = (y + d) % ny
                rc(
                    r["UZ"].at[level], U.at[1 + ly + level, rows(slot, ch)], d_sems[ly + level], dev(z, to, c, x)
                ).start()
            U[1 + ly + level, rows(slot, ch), :] = r["UZ"][level]
        leave(chunks(ny - 1), d_sems[ly + level], bit(z, level) == 1)

    def shared(first, last):
        for level in range(first, last):
            own_bit = bit(y, level) if level < ly else bit(z, level - ly)
            when(own_bit == 1, rc(chunks(ny - 1), chunks(ny - 1), d_sems[level], partner).wait_recv)
        part = U.at[1 + first:1 + last, half]
        cp = rc(part, part, sems.take(), partner)
        cp.start()
        pending.append((None, cp))
        return cp

    share_y = shared(0, ly)

    lax.fori_loop(0, 1, local_pair, 0)

    gb.wait_recv()
    for level in range(ly + lz):
        both = r["Gf"][1 + level, half, :] + pG[1 + level, half, :].astype(F32)
        r["GS"][level] = both.astype(BF16)
    e_sems = [sems.take() for _ in range(ly + lz)]
    for level in range(ly + lz):
        own_bit = bit(y, level) if level < ly else bit(z, level - ly)
        leave(chunks(ny - 1), e_sems[level], own_bit == 1)

        @pl.when(own_bit == 1)
        def _():
            for d in y_order:
                to = (y + d) % ny
                rc(
                    r["GS"].at[level, rows(to, ch)], r["rD"].at[y, level], e_sems[level], dev(z, to, c, x)
                ).start()
            r["rD"][y, level] = r["GS"][level, rows(y, ch), :]

    lax.fori_loop(1, 4, local_pair, 0, unroll=3)

    def states_of(p, first, last):
        return jnp.concatenate([spread_pair(U[m, rows(p, 128), :]) for m in range(first, last)], 0)

    def add_levels(p, back, first, last):
        count = last - first
        q2 = q[:, l128(p)].astype(F32)
        terms = [split_in_two(back[:, m * 128:(m + 1) * 128] * q2) for m in range(count)]
        out_row = lax.broadcasted_iota(jnp.int32, (count * 256, 128), 0)
        out_col = lax.broadcasted_iota(jnp.int32, (count * 256, 128), 1)
        table = jnp.where(
            out_col == (2 * p + (out_row % 128) // DK) * LEVELS + BASE + first + out_row // 256, 1.0, 0.0
        ).astype(BF16)
        return mm(jnp.concatenate(terms, 1), table)

    def add_states(p, back, wide, first, last):
        columns = slice(first * 128, last * 128)
        out = r["oacc"][:, l256(p)] + mm(r["sQ"][p, :, columns], wide)
        dq2 = r["dq"][:, l128(p)]
        for m in range(last - first):
            at = slice((first + m) * 128, (first + m + 1) * 128)
            dq2 = dq2 + r["lw2"][p, :, at].astype(F32) * back[:, m * 128:(m + 1) * 128]
        return out, dq2

    def near_levels(p, carry):
        wide = states_of(p, 0, 1 + ly)
        back = dot(g[:, l256(p)], wide, 1, 1)
        carry = carry + add_levels(p, back, 0, 1 + ly)
        out, dq2 = add_states(p, back, wide, 0, 1 + ly)
        r["oacc"][:, l256(p)] = out
        r["dq"][:, l128(p)] = dq2
        return carry

    def far_levels(p, carry):
        return carry + add_levels(p, dot(g[:, l256(p)], states_of(p, 1 + ly, nl), 1, 1), 1 + ly, nl)

    def far_states(p, carry):
        wide = states_of(p, 1 + ly, nl)
        out, dq2 = add_states(p, dot(g[:, l256(p)], wide, 1, 1), wide, 1 + ly, nl)
        r["o_out"][:, l256(p)] = out.astype(BF16)
        r["o_dq"][:, l128(p)] = dq2.astype(BF16)
        return carry

    def send_levels(gl, part, place):
        gp = (gl * r["sig"][...]).astype(BF16)
        sides = jnp.concatenate([gp[:128], gp[128:]], 1)
        place[x] = mm(sides, r["swap"][:, part * 128:(part + 1) * 128]).astype(BF16)
        sem = sems.take()
        for d in x_order:
            to = (x + d) % nx
            rc(place.at[x], place.at[x], sem, dev(z, y, c, to)).start()
        leave(place.at[0:nx - 1], sem)
        return sem

    low_sem = send_levels(r["gl"][...], 0, r["gpL"])

    share_y.wait_recv()
    near = lax.fori_loop(0, 4, near_levels, r["gl"][...], unroll=4)
    r["gl"][...] = near
    share_z = shared(ly, ly + lz)
    share_z.wait_recv()
    gl = lax.fori_loop(0, 4, far_levels, r["gl"][...], unroll=4)
    high_sem = send_levels(gl, 1, r["gpH"])

    lax.fori_loop(0, 4, far_states, 0, unroll=4)

    arrive(r["gpL"].at[0:nx - 1], low_sem)
    arrive(r["gpH"].at[0:nx - 1], high_sem)
    for j in range(nx):
        sides = jnp.concatenate([r["gpL"][j], r["gpH"][j]], 1)
        sides = dot(sides, r["swap"][...], 1, 1).astype(BF16)
        r["gpA"][j] = jnp.concatenate([sides[:, :128], sides[:, 128:]], 0)
    def left(j):
        return hid[...] if j % 2 == 0 else r["hidp"][...]

    for j in range(nq):
        r["dws"][j] = dot(left(j), r["gpA"][(1 - c) * nq + j], 0, 0).astype(BF16)
    w_copy = rc(r["dws"], r["rDW"], sems.take(), partner)
    w_copy.start()
    pending.append((None, w_copy))
    own_dw = [dot(left(j), r["gpA"][c * nq + j], 0, 0) for j in range(nq)]

    for level in range(ly + lz):
        if level >= ly:
            when(bit(z, level - ly) == 1, rc(chunks(ny - 1), chunks(ny - 1), e_sems[level], partner).wait_recv)
            continue
        for own in range(2):
            n = ny // 2 - own
            if n:
                when(bit(y, level) == own, rc(chunks(n), chunks(n), e_sems[level], partner).wait_recv)
    for level in range(lz):
        @pl.when(bit(z, level) == 1)
        def _():
            value = r["rD"][0, ly + level].astype(F32)
            for i in range(1, ny):
                value = value + r["rD"][i, ly + level].astype(F32)
            r["GZ"][level] = value.astype(BF16)
    f_sem = sems.take()
    for d in range(nz - 1, 0, -1):
        to = (z + nz - d) % nz
        top = 0
        for level in range(lz):
            apart = z // (1 << level) - to // (1 << level)
            top = top + (apart + nz - 1) // nz
        at = (top + lz - 1) % lz
        cp = rc(r["GZ"].at[at], r["rC2"].at[z], f_sem, dev(to, y, c, x))
        when(z >= d, cp.start)
    for at in range(1, nz):
        leave(r["rC2"].at[0:at], f_sem, z == at)

    d_hidden = dot(r["gpA"][0], w[:, 0:128], 1, 1)
    for j in range(1, nx):
        d_hidden = d_hidden + dot(r["gpA"][j], w[:, j * 128:(j + 1) * 128], 1, 1)
    r["o_dh"][...] = d_hidden.astype(BF16)

    def along(axis, d):
        return (dev((z + d) % nz, y, c, x), (z + d) % nz) if axis == 0 else (dev(z, (y + d) % ny, c, x), (y + d) % ny)

    here = (z, y)
    orders = (z_order, y_order)
    counts = (nz, ny)
    w_copy.wait_recv()
    first_sems = [sems.take() for _ in range(nq)]
    for j in range(nq):
        both = own_dw[j] + r["rDW"][j].astype(F32)
        axis = j % 2
        size = 512 // counts[axis]
        for i in range(counts[axis]):
            r[f"dw{j}a"][i] = both[i * size:(i + 1) * size].astype(BF16)
        for d in orders[axis]:
            device, to = along(axis, d)
            rc(r[f"dw{j}a"].at[to], r[f"rd{j}a"].at[here[axis]], first_sems[j], device).start()
        leave(r[f"dw{j}a"].at[0:counts[axis] - 1], first_sems[j])
        r[f"rd{j}a"][here[axis]] = r[f"dw{j}a"][here[axis]]

    for at in range(nz - 1):
        part = r["rC2"].at[0:nz - 1 - at]
        when(z == at, rc(part, part, f_sem, partner).wait_recv)
    r["rC2"][z] = jnp.zeros((ch, 128), BF16)
    for i in range(nz):
        @pl.when(i < z)
        def _():
            r["rC2"][i] = jnp.zeros((ch, 128), BF16)
    from_z = r["rC2"][0].astype(F32)
    for i in range(1, nz):
        from_z = from_z + r["rC2"][i].astype(F32)
    for i in range(ny):
        value = from_z
        for later in range(i + 1, ny):
            value = value + r["rD"][later, (i ^ later).bit_length() - 1].astype(F32)
        r["R"][i] = value.astype(BF16)
    h_sem = sems.take()
    for d in y_order:
        to = (y + d) % ny
        rc(r["R"].at[to], r["adj"].at[rows(slot, ch)], h_sem, dev(z, to, c, x)).start()
    leave(chunks(ny - 1), h_sem)
    r["adj"][rows(slot, ch), :] = r["R"][y]

    second_sems = [sems.take() for _ in range(nq)]
    keep = ry // 2
    for j in range(nq):
        axis = j % 2
        arrive(r[f"rd{j}a"].at[0:counts[axis] - 1], first_sems[j])
        value = r[f"rd{j}a"][0].astype(F32)
        for i in range(1, counts[axis]):
            value = value + r[f"rd{j}a"][i].astype(F32)
        axis = 1 - axis
        count = counts[axis]
        for i in range(count):
            for t in range(2):
                r[f"dw{j}b"][2 * i + t] = value[i * ry + t * keep:i * ry + (t + 1) * keep]
        place = r[f"rd{j}b"].at[c * count + here[axis]]
        for d in [*orders[axis], 0]:
            spot = (here[axis] + d) % count
            for t in (1 - c, c)[:2 if d else 1]:
                device = dev(spot, y, t, x) if axis == 0 else dev(z, spot, t, x)
                rc(r[f"dw{j}b"].at[2 * spot + t], place, second_sems[j], device).start()
        leave(r[f"dw{j}b"].at[0:2 * count - 1], second_sems[j])
        r[f"rd{j}b"][c * count + here[axis]] = r[f"dw{j}b"][2 * here[axis] + c]

    arrive(chunks(ny - 1), h_sem)
    adj_share = rc(r["adj"].at[half], r["adj"].at[half], sems.take(), partner)
    adj_share.start()
    pending.append((None, adj_share))

    loaded("dst")
    adj_share.wait_recv()
    ga.wait_recv()
    first = (1 - c).astype(F32)

    def finish(p, carry):
        at = rows(p, 128)
        total = r["dst"][at, :] + r["adj"][at, :].astype(F32) + pG[0, at, :].astype(F32) * first
        wide = spread_pair(total.astype(BF16))
        dk2 = r["dk"][:, l128(p)] + dot(v[:, l256(p)], wide, 1, 1)
        r["o_dk"][:, l128(p)] = dk2.astype(BF16)
        dv2 = r["dv"][:, l256(p)] + mm(k[:, l128(p)], wide)
        r["o_dv"][:, l256(p)] = dv2.astype(BF16)
        return carry

    lax.fori_loop(0, 4, finish, 0, unroll=4)

    for j in range(nq):
        count = counts[1 - j % 2]
        arrive(r[f"rd{j}b"].at[0:2 * count - 1], second_sems[j])
        for t in range(2):
            value = r[f"rd{j}b"][t * count]
            for i in range(1, count):
                value = value + r[f"rd{j}b"][t * count + i]
            r["o_dw"][:, (t * nq + j) * 128:(t * nq + j + 1) * 128] = value

    assert sems.used == r["send"].shape[0]
    for cond, cp in pending:
        if cond is None:
            cp.wait_send()
        else:
            @pl.when(cond)
            def _():
                cp.wait_send()


def write_out(*refs):
    count = len(refs) // 2
    sem = refs[-1]
    copies = [pltpu.make_async_copy(refs[i], refs[count + i], sem.at[i]) for i in range(count)]
    for cp in copies:
        cp.start()
    for cp in copies:
        cp.wait()


def build(mesh, nz, ny):
    nx = mesh.shape["head"]
    ly, lz = ny.bit_length() - 1, nz.bit_length() - 1
    nl = 1 + ly + lz
    ch = T // ny
    nq = nx // 2
    rz = 512 // nz
    ry = rz // ny
    n_sem = 14 + 2 * (ly + lz) + 2 * nq
    select, member, level = segment_tables()
    levels_of = np.concatenate([level, np.full((128,), 8, np.int32)])[None]
    vm = pltpu.VMEM
    wide = nx * 128
    scratch = [
        vm((nx, T, 128), F32), vm((nx, T, 128), F32),
        vm((512, 128), BF16), vm((512, 128), F32), vm((512, 128), BF16), vm((T, 128), BF16),
        vm((ny, ch, 128), BF16), vm((max(ly, 1), max(ny // 2, 1), ch, 128), BF16), vm((ch, 128), BF16),
        vm((nz, ch, 128), BF16), vm((lz, ch, 128), BF16), vm((nl, 512, 128), BF16),
        vm((4, T, nl * 128), BF16), vm((4, T, nl * 128), BF16),
        vm((nl, 512, 128), BF16), vm((nl, 512, 128), F32), vm((nl, 512, 128), BF16), vm((nl - 1, T, 128), BF16),
        vm((ny, nl - 1, ch, 128), BF16), vm((lz, ch, 128), BF16), vm((nz, ch, 128), BF16),
        vm((ny, ch, 128), BF16), vm((512, 128), BF16),
        vm((T, 1024), F32), vm((T, 512), F32), vm((T, 512), F32), vm((T, 1024), F32),
        vm((T, 128), F32), vm((T, 128), F32), vm((T, 256), BF16),
        vm((nx, T, 128), BF16),
        vm((nq, 512, 128), BF16), vm((nq, 512, 128), BF16),
        vm((nz, rz, 128), BF16), vm((nz, rz, 128), BF16),
        vm((ny, 512 // ny, 128), BF16), vm((ny, 512 // ny, 128), BF16),
        vm((2 * ny, ry // 2, 128), F32), vm((2 * ny, ry // 2, 128), F32),
        vm((2 * nz, ry // 2, 128), F32), vm((2 * nz, ry // 2, 128), F32),
        vm((T, 512), BF16), vm((512, wide), BF16), vm((T, 512), BF16), vm((T, 512), BF16),
        vm((T, 1024), BF16), vm((T, 1024), BF16), vm((512, 128), F32),
        vm((T, 256), BF16), vm((T, 128), BF16), vm((1, 384), jnp.int32),
        vm((8, 384, 128), F32), vm((8, 384, 128), F32), vm((T, 512), BF16),
        vm((T, T), BF16), vm((nx, 128, 128), BF16), vm((nx, 128, 128), BF16),
        pltpu.SemaphoreType.DMA((n_sem,)), pltpu.SemaphoreType.DMA((n_sem,)), pltpu.SemaphoreType.DMA((10,)),
    ]

    results = [
        jax.ShapeDtypeStruct((T, 1024), BF16),
        jax.ShapeDtypeStruct((T, 512), BF16),
        jax.ShapeDtypeStruct((T, 512), BF16),
        jax.ShapeDtypeStruct((T, 1024), BF16),
        jax.ShapeDtypeStruct((T, 512), BF16),
        jax.ShapeDtypeStruct((ry // 2, wide), F32),
    ]

    def step(hidden, w, q, k, v, g, d_state):
        operands = (
            hidden, w, q, k, v, g, d_state.reshape(512, DV),
            jnp.asarray(select, BF16), jnp.asarray(member, BF16), jnp.asarray(levels_of),
        )
        outs = pl.pallas_call(
            functools.partial(kernel, (nz, ny, nx, ly, lz)),
            out_shape=[pltpu.VMEM(a.shape, a.dtype) for a in results],
            in_specs=[pl.BlockSpec(memory_space=pltpu.HBM)] * 10,
            out_specs=[pl.BlockSpec(memory_space=pltpu.VMEM)] * 6,
            scratch_shapes=scratch,
            compiler_params=pltpu.CompilerParams(
                collective_id=0, has_side_effects=True, vmem_limit_bytes=36 * 1024 * 1024
            ),
        )(
            *(pltpu.with_memory_space_constraint(a, pltpu.HBM) for a in operands)
        )
        return pl.pallas_call(
            write_out,
            out_shape=results,
            in_specs=[pl.BlockSpec(memory_space=pltpu.VMEM)] * 6,
            out_specs=[pl.BlockSpec(memory_space=pltpu.HBM)] * 6,
            scratch_shapes=[pltpu.SemaphoreType.DMA((6,))],
            compiler_params=pltpu.CompilerParams(vmem_limit_bytes=8 * 1024 * 1024),
        )(*outs)

    both = P("seq", "head")
    return jax.shard_map(
        step,
        mesh=mesh,
        in_specs=(both, P("head", None), both, both, both, both, P("head", None, None)),
        out_specs=(both, both, both, both, both, P(("head", "seq"), None)),
        check_vma=False,
    )


def solution(mesh):
    return build(mesh, 8, 8)
```

```python
import functools

import jax
import jax.numpy as jnp
import numpy as np
from jax import lax
from jax.experimental import pallas as pl
from jax.experimental.pallas import tpu as pltpu
from jax.sharding import PartitionSpec as P

DK = 64
DV = 128
LEVELS = 16
BASE = 9
T = 256
F32 = jnp.float32
BF16 = jnp.bfloat16


def dot(a, b, da, db):
    return lax.dot_general(a, b, (((da,), (db,)), ((), ())), preferred_element_type=F32)


def mm(a, b):
    return dot(a, b, 1, 0)


def segment_tables():
    select = np.zeros((128, 256), np.float32)
    member = np.zeros((256, 128), np.float32)
    level = np.full((256,), 99, np.int32)
    level[:128] = 0
    rows = np.arange(128)
    select[rows, rows] = 1.0
    member[rows, rows] = 1.0
    col = 128
    for k in range(7):
        for i in range(64 >> k):
            select[:, col] = (rows >> k) == 2 * i + 1
            member[col, :] = (rows >> k) == 2 * i
            level[col] = k + 1
            col += 1
    return np.concatenate([select, select], 0), member, level


class Sems:
    def __init__(self, send, recv):
        self.send, self.recv, self.used = send, recv, 0

    def take(self):
        at = self.used
        self.used += 1
        return (None if self.send is None else (self.send.at[at], self.recv.at[at]))


def kernel(cfg, *refs):
    nz, ny, nx, ly, lz = cfg
    nl = 1 + ly + lz
    ch = T // ny
    nq = nx // 2
    rz = 512 // nz
    ry = rz // ny
    names = (
        "in0", "in1", "in2", "in3", "in4", "in5", "in6", "in7", "in8", "in9", "o_out", "o_dq", "o_dk", "o_dv", "o_dh", "o_dw",
        "part", "rX", "kv", "kvf", "pk", "S", "rB", "tY", "TT", "rC", "UZ", "U", "sQ", "lw2", "G", "Gf", "pG", "GS",
        "rD", "GZ", "rC2", "R", "adj", "oacc", "dq", "dk", "dv", "gl", "sig", "lwb", "gpA", "dws", "rDW", "dw0a", "rd0a", "dw1a", "rd1a",
        "dw0b", "rd0b", "dw1b", "rd1b",  "hid", "w", "q", "k", "v", "g", "dst", "sel", "mem", "lev",
        "scs", "gms", "hidp", "swap", "gpL", "gpH", "send", "recv", "load",
    )
    r = dict(zip(names, refs, strict=True))
    hid, w, q, k, v, g = (r[n] for n in ("hid", "w", "q", "k", "v", "g"))
    sems = Sems(r["send"], r["recv"])

    s = lax.axis_index("seq")
    x = lax.axis_index("head")
    c = s % 2
    y = (s // 2) % ny
    z = s // (2 * ny)

    def dev(zz, yy, cc, xx):
        return (zz * (2 * ny) + yy * 2 + cc, xx)

    def rc(src, dst, sem, to):
        return pltpu.make_async_remote_copy(
            src_ref=src, dst_ref=dst, send_sem=sem[0], recv_sem=sem[1], device_id=to,
            device_id_type=pl.DeviceIdType.MESH,
        )

    partner = dev(z, y, 1 - c, x)
    y_order = sorted(range(1, ny), key=lambda d: -min(d, ny - d))
    z_order = sorted(range(1, nz), key=lambda d: -min(d, nz - d))
    x_order = sorted(range(1, nx), key=lambda d: -min(d, nx - d))
    pending = []

    def arrive(ref, sem):
        rc(ref, ref, sem, partner).wait_recv()

    def leave(ref, sem, cond=None):
        pending.append((cond, rc(ref, ref, sem, partner)))

    def chunks(n):
        return r["rB"].at[pl.ds(0, n)]

    def when(cond, action):
        if cond is None:
            action()
        else:
            pl.when(cond)(action)

    def bit(value, j):
        return (value // (1 << j)) % 2

    def rows(at, count):
        return pl.ds(pl.multiple_of(at * count, count), count)

    arrays = ("hid", "w", "q", "k", "v", "g", "dst", "sel", "mem", "lev")
    loads = {n: pltpu.make_async_copy(r[f"in{i}"], r[n], r["load"].at[i]) for i, n in enumerate(arrays)}

    def loaded(*wanted):
        for n in wanted:
            loads[n].wait()

    U, G, pG = r["U"], r["G"], r["pG"]
    barrier = pltpu.get_barrier_semaphore()
    peers = [partner]
    peers += [dev(z, y, c, (x + d) % nx) for d in x_order]
    for t in (c, 1 - c):
        peers += [dev(z, (y + d) % ny, t, x) for d in y_order]
        peers += [dev((z + d) % nz, y, t, x) for d in z_order]
    for peer in peers:
        pl.semaphore_signal(barrier, inc=1, device_id=peer, device_id_type=pl.DeviceIdType.MESH)
    for n in ("k", "v", "hid", "w", "q", "g", "mem", "sel", "lev", "dst"):
        loads[n].start()
    for level in range(nl):
        U[level] = jnp.zeros((512, 128), BF16)

    lane = lax.broadcasted_iota(jnp.int32, (1, 128), 1)
    low = lane < DK

    def pair_rows(full):
        return jnp.concatenate([full[:DK, :128], full[DK:, 128:]], 0)

    def spread_pair(block):
        zero = jnp.zeros((DK, 128), block.dtype)
        left = jnp.concatenate([block[:DK], zero], 0)
        right = jnp.concatenate([zero, block[DK:]], 0)
        return jnp.concatenate([left, right], 1)

    def l128(p):
        return pl.ds(pl.multiple_of(p * 128, 128), 128)

    def l256(p):
        return pl.ds(pl.multiple_of(p * 256, 256), 256)

    loaded("k", "v")
    for p in range(4):
        full = dot(k[:, l128(p)], v[:, l256(p)], 0, 0)
        state = pair_rows(full)
        r["kvf"][pl.ds(p * 128, 128), :] = state
        r["kv"][pl.ds(p * 128, 128), :] = state.astype(BF16)
    loaded("hid", "w")
    for j in range(nx):
        r["part"][j] = mm(hid[...], w[:, pl.ds(j * 128, 128)])

    pl.semaphore_wait(barrier, len(peers))

    a_copy = rc(r["kv"], r["pk"], sems.take(), partner)
    a_copy.start()
    pending.append((None, a_copy))
    x_sem = sems.take()
    for d in x_order:
        to = (x + d) % nx
        rc(r["part"].at[to], r["rX"].at[x], x_sem, dev(z, y, c, to)).start()
    leave(r["part"].at[0:nx - 1], x_sem)

    src = lax.broadcasted_iota(jnp.int32, (512, 512), 0)
    col = lax.broadcasted_iota(jnp.int32, (512, 512), 1)
    wanted = ((col // ry) % nz) * rz + (col // (nz * ry)) * ry + col % ry
    r["hidp"][...] = mm(hid[...], jnp.where(src == wanted, 1.0, 0.0).astype(BF16)).astype(BF16)

    src = lax.broadcasted_iota(jnp.int32, (T, T), 0)
    col = lax.broadcasted_iota(jnp.int32, (T, T), 1)
    level = src % LEVELS
    packed = (level // 8) * 128 + (src // 128) * 64 + ((src % 128) // LEVELS) * 8 + level % 8
    r["swap"][...] = jnp.where(col == packed, 1.0, 0.0).astype(BF16)

    a_copy.wait_recv()
    half = rows(c, T)
    mine = r["kvf"][half, :] + r["pk"][half, :].astype(F32)
    r["S"][...] = mine.astype(BF16)
    U[0] = (r["pk"][...].astype(F32) * c.astype(F32)).astype(BF16)
    b_sem = sems.take()
    for d in y_order:
        to = (y + d) % ny
        rc(r["S"].at[rows(to, ch)], r["rB"].at[y], b_sem, dev(z, to, c, x)).start()
    leave(chunks(ny - 1), b_sem)
    r["rB"][y] = r["S"][rows(y, ch), :]

    loaded("q", "g", "mem", "sel", "lev")
    head_row = lax.broadcasted_iota(jnp.int32, (128, 384), 0)

    def level_columns(head):
        return jnp.where(head_row == head * LEVELS + r["lev"][...], 1.0, 0.0).astype(BF16)

    def split_in_two(value):
        upper_part = value.astype(BF16)
        return jnp.concatenate([upper_part, (value - upper_part.astype(F32)).astype(BF16)], 1)

    def scores(p, carry):
        q2 = q[:, l128(p)]
        k2 = k[:, l128(p)]
        member = r["mem"][...]
        gl = carry
        for i in range(2):
            mask = low if i == 0 else jnp.logical_not(low)
            qh = jnp.where(mask, q2, jnp.zeros_like(q2))
            at = pl.ds(pl.multiple_of(p * 256 + i * 128, 128), 128)
            sc = dot(qh, k2, 1, 1)
            gm = dot(g[:, at], v[:, at], 1, 1)
            sc = jnp.concatenate([sc[:128, :128], sc[128:, 128:], sc[128:, :128]], 0)
            gm = jnp.concatenate([gm[:128, :128], gm[128:, 128:], gm[128:, :128]], 0)
            r["scs"][2 * p + i] = sc
            r["gms"][2 * p + i] = gm
            table = level_columns(2 * p + i)
            prod = split_in_two(sc * gm)
            near = dot(prod[:256], jnp.concatenate([member, member], 1), 1, 1)
            near = near.astype(BF16) * r["sel"][...]
            gl = gl + dot(near, table[:, :256], 1, 1)
            far = dot(prod[256:], jnp.concatenate([table[:, 256:], table[:, 256:]], 1), 1, 1)
            gl = gl + jnp.concatenate([jnp.zeros((128, 128), F32), far], 0)
        return gl

    r["gl"][...] = lax.fori_loop(0, 4, scores, jnp.zeros((T, 128), F32), unroll=4)

    arrive(chunks(ny - 1), b_sem)
    sums = [r["rB"][i].astype(F32) for i in range(ny)]
    for j in range(1, ly):
        sums = [sums[2 * i] + sums[2 * i + 1] for i in range(len(sums) // 2)]
        for i, value in enumerate(sums):
            r["tY"][j, i] = value.astype(BF16)
    r["TT"][...] = (sums[0] + sums[1]).astype(BF16)
    c_sem = sems.take()
    for d in range(nz - 1, 0, -1):
        to = (z + d) % nz
        cp = rc(r["TT"], r["rC"].at[z], c_sem, dev(to, y, c, x))
        when(z + d < nz, cp.start)
    for at in range(nz - 1):
        leave(r["rC"].at[0:nz - 1 - at], c_sem, z == at)

    def y_source(level, target):
        at = target // (1 << level) - 1
        at = (at + ny) % ny
        return r["rB"].at[at] if level == 0 else r["tY"].at[level, at]

    slot = c * ny + y
    d_sems = [sems.take() for _ in range(ly + lz)]
    for level in range(ly):
        for d in y_order:
            to = (y + d) % ny
            cp = rc(
                y_source(level, to), U.at[1 + level, rows(slot, ch)], d_sems[level], dev(z, to, c, x)
            )
            when(bit(to, level) == 1, cp.start)
        for own in range(2):
            if ny // 2 - own:
                leave(chunks(ny // 2 - own), d_sems[level], bit(y, level) == own)

        @pl.when(bit(y, level) == 1)
        def _():
            U[1 + level, rows(slot, ch), :] = y_source(level, y)[...]

    arrive(r["rX"].at[0:nx - 1], x_sem)
    r["rX"][x] = r["part"][x]
    projected = r["rX"][0]
    for j in range(1, nx):
        projected = projected + r["rX"][j]
    weights = jnp.maximum(projected, 0.0) + jnp.log1p(jnp.exp(-jnp.abs(projected)))
    upper_part = weights.astype(BF16)
    rest = (weights - upper_part.astype(F32)).astype(BF16)
    r["lwb"][...] = jnp.concatenate([upper_part, rest], 1)
    r["sig"][...] = jax.nn.sigmoid(projected)

    row_id = lax.broadcasted_iota(jnp.int32, (128, nl * 128), 0)
    col_id = lax.broadcasted_iota(jnp.int32, (128, nl * 128), 1)
    col_level = BASE + col_id // 128
    col_head = (col_id % 128) // DK

    def upper_table(p):
        return jnp.where(row_id == (2 * p + col_head) * LEVELS + col_level, 1.0, 0.0).astype(BF16)

    def grad_states(p, carry):
        table = upper_table(p)
        wide = mm(r["lwb"][...], jnp.concatenate([table, table], 0))
        r["lw2"][p] = wide.astype(BF16)
        q2 = q[:, l128(p)].astype(F32)
        gg = g[:, l256(p)]
        for m in range(nl):
            scaled = (wide[:, m * 128:(m + 1) * 128] * q2).astype(BF16)
            r["sQ"][p, :, m * 128:(m + 1) * 128] = scaled
            state = pair_rows(dot(scaled, gg, 0, 0))
            r["Gf"][m, rows(p, 128), :] = state
            G[m, rows(p, 128), :] = state.astype(BF16)
        return carry

    lax.fori_loop(0, 4, grad_states, 0, unroll=4)
    ga = rc(G.at[0], pG.at[0], sems.take(), partner)
    ga.start()
    pending.append((None, ga))
    other = rows(1 - c, T)
    gb = rc(G.at[1:nl, other], pG.at[1:nl, other], sems.take(), partner)
    gb.start()
    pending.append((None, gb))

    def local_pair(p, carry):
        q2 = q[:, l128(p)]
        k2 = k[:, l128(p)]
        select = r["sel"][...]
        member = r["mem"][...]
        dq2 = jnp.zeros((T, 128), F32)
        dk2 = jnp.zeros((T, 128), F32)
        zero = jnp.zeros((128, 128), BF16)
        for i in range(2):
            mask = low if i == 0 else jnp.logical_not(low)
            qh = jnp.where(mask, q2, jnp.zeros_like(q2))
            kh = jnp.where(mask, k2, jnp.zeros_like(k2))
            at = pl.ds(pl.multiple_of(p * 256 + i * 128, 128), 128)
            vh = v[:, at]
            gh = g[:, at]
            table = level_columns(2 * p + i)
            wide = mm(r["lwb"][...], jnp.concatenate([table, table], 0))
            chosen = wide[:, :256].astype(BF16) * select
            spread = mm(chosen, member)
            far = wide[128:, 256:]
            both = jnp.concatenate([spread, far], 0)
            mixed = (r["scs"][2 * p + i] * both).astype(BF16)
            gs = (r["gms"][2 * p + i] * both).astype(BF16)

            def square(block):
                top = jnp.concatenate([block[:128], zero], 1)
                return jnp.concatenate([top, jnp.concatenate([block[256:], block[128:256]], 1)], 0)

            mixed = square(mixed)
            gs = square(gs)
            r["oacc"][:, at] = mm(mixed, vh)
            r["dv"][:, at] = dot(mixed, gh, 0, 0)
            dq2 = dq2 + mm(gs, kh)
            dk2 = dk2 + dot(gs, qh, 0, 0)
        r["dq"][:, l128(p)] = dq2
        r["dk"][:, l128(p)] = dk2
        return carry

    for at in range(1, nz):
        when(z == at, rc(r["rC"].at[0:at], r["rC"].at[0:at], c_sem, partner).wait_recv)
    for level in range(lz):
        @pl.when(bit(z, level) == 1)
        def _():
            start = (z // (1 << level) - 1) * (1 << level)
            value = r["rC"][start].astype(F32)
            for i in range(1, 1 << level):
                value = value + r["rC"][start + i].astype(F32)
            r["UZ"][level] = value.astype(BF16)
            for d in y_order:
                to = (y + d) % ny
                rc(
                    r["UZ"].at[level], U.at[1 + ly + level, rows(slot, ch)], d_sems[ly + level], dev(z, to, c, x)
                ).start()
            U[1 + ly + level, rows(slot, ch), :] = r["UZ"][level]
        leave(chunks(ny - 1), d_sems[ly + level], bit(z, level) == 1)

    def shared(first, last):
        for level in range(first, last):
            own_bit = bit(y, level) if level < ly else bit(z, level - ly)
            when(own_bit == 1, rc(chunks(ny - 1), chunks(ny - 1), d_sems[level], partner).wait_recv)
        part = U.at[1 + first:1 + last, half]
        cp = rc(part, part, sems.take(), partner)
        cp.start()
        pending.append((None, cp))
        return cp

    share_y = shared(0, ly)

    lax.fori_loop(0, 1, local_pair, 0)

    gb.wait_recv()
    for level in range(ly + lz):
        both = r["Gf"][1 + level, half, :] + pG[1 + level, half, :].astype(F32)
        r["GS"][level] = both.astype(BF16)
    e_sems = [sems.take() for _ in range(ly + lz)]
    for level in range(ly + lz):
        own_bit = bit(y, level) if level < ly else bit(z, level - ly)
        leave(chunks(ny - 1), e_sems[level], own_bit == 1)

        @pl.when(own_bit == 1)
        def _():
            for d in y_order:
                to = (y + d) % ny
                rc(
                    r["GS"].at[level, rows(to, ch)], r["rD"].at[y, level], e_sems[level], dev(z, to, c, x)
                ).start()
            r["rD"][y, level] = r["GS"][level, rows(y, ch), :]

    lax.fori_loop(1, 4, local_pair, 0, unroll=3)

    def states_of(p, first, last):
        return jnp.concatenate([spread_pair(U[m, rows(p, 128), :]) for m in range(first, last)], 0)

    def add_levels(p, back, first, last):
        count = last - first
        q2 = q[:, l128(p)].astype(F32)
        terms = [split_in_two(back[:, m * 128:(m + 1) * 128] * q2) for m in range(count)]
        out_row = lax.broadcasted_iota(jnp.int32, (count * 256, 128), 0)
        out_col = lax.broadcasted_iota(jnp.int32, (count * 256, 128), 1)
        table = jnp.where(
            out_col == (2 * p + (out_row % 128) // DK) * LEVELS + BASE + first + out_row // 256, 1.0, 0.0
        ).astype(BF16)
        return mm(jnp.concatenate(terms, 1), table)

    def add_states(p, back, wide, first, last):
        columns = slice(first * 128, last * 128)
        out = r["oacc"][:, l256(p)] + mm(r["sQ"][p, :, columns], wide)
        dq2 = r["dq"][:, l128(p)]
        for m in range(last - first):
            at = slice((first + m) * 128, (first + m + 1) * 128)
            dq2 = dq2 + r["lw2"][p, :, at].astype(F32) * back[:, m * 128:(m + 1) * 128]
        return out, dq2

    def near_levels(p, carry):
        wide = states_of(p, 0, 1 + ly)
        back = dot(g[:, l256(p)], wide, 1, 1)
        carry = carry + add_levels(p, back, 0, 1 + ly)
        out, dq2 = add_states(p, back, wide, 0, 1 + ly)
        r["oacc"][:, l256(p)] = out
        r["dq"][:, l128(p)] = dq2
        return carry

    def far_levels(p, carry):
        return carry + add_levels(p, dot(g[:, l256(p)], states_of(p, 1 + ly, nl), 1, 1), 1 + ly, nl)

    def far_states(p, carry):
        wide = states_of(p, 1 + ly, nl)
        out, dq2 = add_states(p, dot(g[:, l256(p)], wide, 1, 1), wide, 1 + ly, nl)
        r["o_out"][:, l256(p)] = out.astype(BF16)
        r["o_dq"][:, l128(p)] = dq2.astype(BF16)
        return carry

    def send_levels(gl, part, place):
        gp = (gl * r["sig"][...]).astype(BF16)
        sides = jnp.concatenate([gp[:128], gp[128:]], 1)
        place[x] = mm(sides, r["swap"][:, part * 128:(part + 1) * 128]).astype(BF16)
        sem = sems.take()
        for d in x_order:
            to = (x + d) % nx
            rc(place.at[x], place.at[x], sem, dev(z, y, c, to)).start()
        leave(place.at[0:nx - 1], sem)
        return sem

    low_sem = send_levels(r["gl"][...], 0, r["gpL"])

    share_y.wait_recv()
    near = lax.fori_loop(0, 4, near_levels, r["gl"][...], unroll=4)
    r["gl"][...] = near
    share_z = shared(ly, ly + lz)
    gl = r["gl"][...]
    for i in range(2):
        gl = far_levels(2 * c + i, gl)
    share_z.wait_recv()
    for i in range(2):
        gl = far_levels(2 * (1 - c) + i, gl)
    high_sem = send_levels(gl, 1, r["gpH"])

    lax.fori_loop(0, 4, far_states, 0, unroll=4)

    arrive(r["gpL"].at[0:nx - 1], low_sem)
    arrive(r["gpH"].at[0:nx - 1], high_sem)
    for j in range(nx):
        sides = jnp.concatenate([r["gpL"][j], r["gpH"][j]], 1)
        sides = dot(sides, r["swap"][...], 1, 1).astype(BF16)
        r["gpA"][j] = jnp.concatenate([sides[:, :128], sides[:, 128:]], 0)
    def left(j):
        return hid[...] if j % 2 == 0 else r["hidp"][...]

    for j in range(nq):
        r["dws"][j] = dot(left(j), r["gpA"][(1 - c) * nq + j], 0, 0).astype(BF16)
    w_copy = rc(r["dws"], r["rDW"], sems.take(), partner)
    w_copy.start()
    pending.append((None, w_copy))
    own_dw = [dot(left(j), r["gpA"][c * nq + j], 0, 0) for j in range(nq)]

    for level in range(ly + lz):
        if level >= ly:
            when(bit(z, level - ly) == 1, rc(chunks(ny - 1), chunks(ny - 1), e_sems[level], partner).wait_recv)
            continue
        for own in range(2):
            n = ny // 2 - own
            if n:
                when(bit(y, level) == own, rc(chunks(n), chunks(n), e_sems[level], partner).wait_recv)
    for level in range(lz):
        @pl.when(bit(z, level) == 1)
        def _():
            value = r["rD"][0, ly + level].astype(F32)
            for i in range(1, ny):
                value = value + r["rD"][i, ly + level].astype(F32)
            r["GZ"][level] = value.astype(BF16)
    f_sem = sems.take()
    for d in range(nz - 1, 0, -1):
        to = (z + nz - d) % nz
        top = 0
        for level in range(lz):
            apart = z // (1 << level) - to // (1 << level)
            top = top + (apart + nz - 1) // nz
        at = (top + lz - 1) % lz
        cp = rc(r["GZ"].at[at], r["rC2"].at[z], f_sem, dev(to, y, c, x))
        when(z >= d, cp.start)
    for at in range(1, nz):
        leave(r["rC2"].at[0:at], f_sem, z == at)

    d_hidden = dot(r["gpA"][0], w[:, 0:128], 1, 1)
    for j in range(1, nx):
        d_hidden = d_hidden + dot(r["gpA"][j], w[:, j * 128:(j + 1) * 128], 1, 1)
    r["o_dh"][...] = d_hidden.astype(BF16)

    def along(axis, d):
        return (dev((z + d) % nz, y, c, x), (z + d) % nz) if axis == 0 else (dev(z, (y + d) % ny, c, x), (y + d) % ny)

    here = (z, y)
    orders = (z_order, y_order)
    counts = (nz, ny)
    w_copy.wait_recv()
    first_sems = [sems.take() for _ in range(nq)]
    for j in range(nq):
        both = own_dw[j] + r["rDW"][j].astype(F32)
        axis = j % 2
        size = 512 // counts[axis]
        for i in range(counts[axis]):
            r[f"dw{j}a"][i] = both[i * size:(i + 1) * size].astype(BF16)
        for d in orders[axis]:
            device, to = along(axis, d)
            rc(r[f"dw{j}a"].at[to], r[f"rd{j}a"].at[here[axis]], first_sems[j], device).start()
        leave(r[f"dw{j}a"].at[0:counts[axis] - 1], first_sems[j])
        r[f"rd{j}a"][here[axis]] = r[f"dw{j}a"][here[axis]]

    for at in range(nz - 1):
        part = r["rC2"].at[0:nz - 1 - at]
        when(z == at, rc(part, part, f_sem, partner).wait_recv)
    r["rC2"][z] = jnp.zeros((ch, 128), BF16)
    for i in range(nz):
        @pl.when(i < z)
        def _():
            r["rC2"][i] = jnp.zeros((ch, 128), BF16)
    from_z = r["rC2"][0].astype(F32)
    for i in range(1, nz):
        from_z = from_z + r["rC2"][i].astype(F32)
    for i in range(ny):
        value = from_z
        for later in range(i + 1, ny):
            value = value + r["rD"][later, (i ^ later).bit_length() - 1].astype(F32)
        r["R"][i] = value.astype(BF16)
    h_sem = sems.take()
    for d in y_order:
        to = (y + d) % ny
        rc(r["R"].at[to], r["adj"].at[rows(slot, ch)], h_sem, dev(z, to, c, x)).start()
    leave(chunks(ny - 1), h_sem)
    r["adj"][rows(slot, ch), :] = r["R"][y]

    second_sems = [sems.take() for _ in range(nq)]
    keep = ry // 2
    for j in range(nq):
        axis = j % 2
        arrive(r[f"rd{j}a"].at[0:counts[axis] - 1], first_sems[j])
        value = r[f"rd{j}a"][0].astype(F32)
        for i in range(1, counts[axis]):
            value = value + r[f"rd{j}a"][i].astype(F32)
        axis = 1 - axis
        count = counts[axis]
        for i in range(count):
            for t in range(2):
                r[f"dw{j}b"][2 * i + t] = value[i * ry + t * keep:i * ry + (t + 1) * keep]
        place = r[f"rd{j}b"].at[c * count + here[axis]]
        for d in [*orders[axis], 0]:
            spot = (here[axis] + d) % count
            for t in (1 - c, c)[:2 if d else 1]:
                device = dev(spot, y, t, x) if axis == 0 else dev(z, spot, t, x)
                rc(r[f"dw{j}b"].at[2 * spot + t], place, second_sems[j], device).start()
        leave(r[f"dw{j}b"].at[0:2 * count - 1], second_sems[j])
        r[f"rd{j}b"][c * count + here[axis]] = r[f"dw{j}b"][2 * here[axis] + c]

    arrive(chunks(ny - 1), h_sem)
    adj_share = rc(r["adj"].at[half], r["adj"].at[half], sems.take(), partner)
    adj_share.start()
    pending.append((None, adj_share))

    loaded("dst")
    ga.wait_recv()
    first = (1 - c).astype(F32)

    def finish(p, carry):
        at = rows(p, 128)
        total = r["dst"][at, :] + r["adj"][at, :].astype(F32) + pG[0, at, :].astype(F32) * first
        wide = spread_pair(total.astype(BF16))
        dk2 = r["dk"][:, l128(p)] + dot(v[:, l256(p)], wide, 1, 1)
        r["o_dk"][:, l128(p)] = dk2.astype(BF16)
        dv2 = r["dv"][:, l256(p)] + mm(k[:, l128(p)], wide)
        r["o_dv"][:, l256(p)] = dv2.astype(BF16)
        return carry

    for i in range(2):
        finish(2 * c + i, 0)
    adj_share.wait_recv()
    for i in range(2):
        finish(2 * (1 - c) + i, 0)

    for j in range(nq):
        count = counts[1 - j % 2]
        arrive(r[f"rd{j}b"].at[0:2 * count - 1], second_sems[j])
        for t in range(2):
            value = r[f"rd{j}b"][t * count]
            for i in range(1, count):
                value = value + r[f"rd{j}b"][t * count + i]
            r["o_dw"][:, (t * nq + j) * 128:(t * nq + j + 1) * 128] = value

    assert sems.used == r["send"].shape[0]
    for cond, cp in pending:
        if cond is None:
            cp.wait_send()
        else:
            @pl.when(cond)
            def _():
                cp.wait_send()


def write_out(*refs):
    count = len(refs) // 2
    sem = refs[-1]
    copies = [pltpu.make_async_copy(refs[i], refs[count + i], sem.at[i]) for i in range(count)]
    for cp in copies:
        cp.start()
    for cp in copies:
        cp.wait()


def build(mesh, nz, ny):
    nx = mesh.shape["head"]
    ly, lz = ny.bit_length() - 1, nz.bit_length() - 1
    nl = 1 + ly + lz
    ch = T // ny
    nq = nx // 2
    rz = 512 // nz
    ry = rz // ny
    n_sem = 14 + 2 * (ly + lz) + 2 * nq
    select, member, level = segment_tables()
    levels_of = np.concatenate([level, np.full((128,), 8, np.int32)])[None]
    vm = pltpu.VMEM
    wide = nx * 128
    scratch = [
        vm((nx, T, 128), F32), vm((nx, T, 128), F32),
        vm((512, 128), BF16), vm((512, 128), F32), vm((512, 128), BF16), vm((T, 128), BF16),
        vm((ny, ch, 128), BF16), vm((max(ly, 1), max(ny // 2, 1), ch, 128), BF16), vm((ch, 128), BF16),
        vm((nz, ch, 128), BF16), vm((lz, ch, 128), BF16), vm((nl, 512, 128), BF16),
        vm((4, T, nl * 128), BF16), vm((4, T, nl * 128), BF16),
        vm((nl, 512, 128), BF16), vm((nl, 512, 128), F32), vm((nl, 512, 128), BF16), vm((nl - 1, T, 128), BF16),
        vm((ny, nl - 1, ch, 128), BF16), vm((lz, ch, 128), BF16), vm((nz, ch, 128), BF16),
        vm((ny, ch, 128), BF16), vm((512, 128), BF16),
        vm((T, 1024), F32), vm((T, 512), F32), vm((T, 512), F32), vm((T, 1024), F32),
        vm((T, 128), F32), vm((T, 128), F32), vm((T, 256), BF16),
        vm((nx, T, 128), BF16),
        vm((nq, 512, 128), BF16), vm((nq, 512, 128), BF16),
        vm((nz, rz, 128), BF16), vm((nz, rz, 128), BF16),
        vm((ny, 512 // ny, 128), BF16), vm((ny, 512 // ny, 128), BF16),
        vm((2 * ny, ry // 2, 128), F32), vm((2 * ny, ry // 2, 128), F32),
        vm((2 * nz, ry // 2, 128), F32), vm((2 * nz, ry // 2, 128), F32),
        vm((T, 512), BF16), vm((512, wide), BF16), vm((T, 512), BF16), vm((T, 512), BF16),
        vm((T, 1024), BF16), vm((T, 1024), BF16), vm((512, 128), F32),
        vm((T, 256), BF16), vm((T, 128), BF16), vm((1, 384), jnp.int32),
        vm((8, 384, 128), F32), vm((8, 384, 128), F32), vm((T, 512), BF16),
        vm((T, T), BF16), vm((nx, 128, 128), BF16), vm((nx, 128, 128), BF16),
        pltpu.SemaphoreType.DMA((n_sem,)), pltpu.SemaphoreType.DMA((n_sem,)), pltpu.SemaphoreType.DMA((10,)),
    ]

    results = [
        jax.ShapeDtypeStruct((T, 1024), BF16),
        jax.ShapeDtypeStruct((T, 512), BF16),
        jax.ShapeDtypeStruct((T, 512), BF16),
        jax.ShapeDtypeStruct((T, 1024), BF16),
        jax.ShapeDtypeStruct((T, 512), BF16),
        jax.ShapeDtypeStruct((ry // 2, wide), F32),
    ]

    def step(hidden, w, q, k, v, g, d_state):
        operands = (
            hidden, w, q, k, v, g, d_state.reshape(512, DV),
            jnp.asarray(select, BF16), jnp.asarray(member, BF16), jnp.asarray(levels_of),
        )
        outs = pl.pallas_call(
            functools.partial(kernel, (nz, ny, nx, ly, lz)),
            out_shape=[pltpu.VMEM(a.shape, a.dtype) for a in results],
            in_specs=[pl.BlockSpec(memory_space=pltpu.HBM)] * 10,
            out_specs=[pl.BlockSpec(memory_space=pltpu.VMEM)] * 6,
            scratch_shapes=scratch,
            compiler_params=pltpu.CompilerParams(
                collective_id=0, has_side_effects=True, vmem_limit_bytes=36 * 1024 * 1024
            ),
        )(
            *(pltpu.with_memory_space_constraint(a, pltpu.HBM) for a in operands)
        )
        return pl.pallas_call(
            write_out,
            out_shape=results,
            in_specs=[pl.BlockSpec(memory_space=pltpu.VMEM)] * 6,
            out_specs=[pl.BlockSpec(memory_space=pltpu.HBM)] * 6,
            scratch_shapes=[pltpu.SemaphoreType.DMA((6,))],
            compiler_params=pltpu.CompilerParams(vmem_limit_bytes=8 * 1024 * 1024),
        )(*outs)

    both = P("seq", "head")
    return jax.shard_map(
        step,
        mesh=mesh,
        in_specs=(both, P("head", None), both, both, both, both, P("head", None, None)),
        out_specs=(both, both, both, both, both, P(("head", "seq"), None)),
        check_vma=False,
    )


def solution(mesh):
    return build(mesh, 8, 8)
```
